256 devices in a mesh: kvp: 32 (over z, x), head: 8 (over y, core).
Axes of the slice: x: 4, y: 4, z: 8, core: 2. Of those that a mesh axis runs over, the one named last changes fastest.
Arguments:
- hidden_in: bfloat16 [16, 8192], P(None, 'kvp'), may hold values from -4 to 4
- attn_gain: bfloat16 [8192], P('kvp'), may hold values from 0.25 to 1.75
- query_key_value_weight: bfloat16 [8192, 8, 1280], P('kvp', 'head'), may hold values from -0.0625 to 0.0625
- k_cache: bfloat16 [8, 2048, 128, 128], P('head', 'kvp'), may hold values from -1200 to 1200
- value_cache: bfloat16 [8, 2048, 128, 128], P('head', 'kvp'), may hold values from -48 to 48
- page_table: int32 [16, 128], P(None, 'kvp'), may hold values from 0 to 63, as said below
- lengths: int32 [16], replicated, may hold values from 4096 to 16384, as said below
- output_weight: bfloat16 [8, 1024, 8192], P('head', None, 'kvp'), may hold values from -0.1875 to 0.1875
- mlp_gain: bfloat16 [8192], P('kvp'), may hold values from 0.099609375 to 1.8984375
- w_in: bfloat16 [8192, 2, 22016], P('kvp', None, 'head'), may hold values from -0.0625 to 0.0625
- w_down: bfloat16 [22016, 8192], P('head', 'kvp'), may hold values from -0.15625 to 0.15625
Outputs:
- next_hidden: bfloat16 [16, 8192], P(None, 'kvp')
The draws below stay inside these ranges and needn't reach their ends.
Inputs may be any that keep to these rules, and one draw needn't show every extreme that they name: `page_table`: within each aligned block of 4 columns, the 16 x 4 entries are a permutation of 0 to 63. `lengths`: in every draw some request has exactly 16384 cached tokens.
All inputs are finite; a program needn't handle non-finite values.
Results may differ from the reference program's by a relative error of at most 0.033.
Values may be sent and summed in bfloat16 or wider, within the bound.
A program may use at most 64 MiB of HBM per device.

```python
import jax
import jax.numpy as jnp
from jax import lax

MODEL_WIDTH = 8192
FF = 22016
HEAD_WIDTH = 128
QUERY_PER_KEY = 8
PAGE_TOKENS = 128
REQUEST_COUNT = 16
PAGES_DEV = 4
KEY_VALUE_HEADS = 8
SLOTS_PER_SPLIT = 64
PAGES = 128
CTX = 16384
N_KVP = 32


def draw_lengths(key, part):
    base_lengths = jax.random.randint(key, (REQUEST_COUNT,), CTX // 4, CTX + 1, dtype=jnp.int32)
    chosen = jax.random.randint(jax.random.fold_in(key, 7), (), 0, REQUEST_COUNT, dtype=jnp.int32)
    return jnp.where(jnp.arange(REQUEST_COUNT, dtype=jnp.int32) == chosen, CTX, base_lengths).astype(jnp.int32)


def draw_page_table(key, part):
    shard_keys = jax.random.split(key, N_KVP)
    orders = jax.vmap(lambda single_key: jax.random.permutation(single_key, REQUEST_COUNT * PAGES_DEV))(shard_keys)
    orders = orders.reshape(N_KVP, REQUEST_COUNT, PAGES_DEV).astype(jnp.int32)
    return jnp.transpose(orders, (1, 0, 2)).reshape(REQUEST_COUNT, N_KVP * PAGES_DEV)


def draw_k_cache(key, part):
    complete_shape = (KEY_VALUE_HEADS, N_KVP * SLOTS_PER_SPLIT, PAGE_TOKENS, HEAD_WIDTH)
    values = jnp.clip(jax.random.normal(key, complete_shape, jnp.float32) * 2.0, -12.0, 12.0)
    return values.astype(jnp.bfloat16)


def levels(key, dims, pieces, low, top_value):
    loudness, own = 1.0, jax.random.fold_in(key, 6)
    for axis_at, parts in pieces:
        heights = jnp.exp(jax.random.uniform(jax.random.fold_in(own, axis_at), (parts,), jnp.float32, low / len(pieces), top_value / len(pieces)))
        loudness = loudness * jnp.repeat(heights, dims[axis_at] // parts).reshape([-1 if axis == axis_at else 1 for axis in range(len(dims))])
    return loudness


def normal_values(stream_key, extent, width, most, cuts=(), held_as=jnp.bfloat16):
    drawn = width * jax.random.normal(stream_key, extent, jnp.float32)
    if cuts:
        drawn = drawn * levels(stream_key, extent, cuts, -0.22, 0.18)
    return jnp.clip(drawn, -most, most).astype(held_as)


def setup_inputs(seed: int = 0) -> dict:
    streams_of = jax.random.split(jax.random.key(seed), 12)
    hidden_in = normal_values(streams_of[0], (REQUEST_COUNT, MODEL_WIDTH), 0.25, 4.0, ((1, 32),))
    attn_gain = jnp.clip(1.0 + 0.15 * jax.random.normal(streams_of[1], (MODEL_WIDTH,), jnp.float32), 0.25, 1.75).astype(jnp.bfloat16)
    query_key_value_weight = normal_values(streams_of[2], (MODEL_WIDTH, KEY_VALUE_HEADS, (QUERY_PER_KEY + 2) * HEAD_WIDTH), MODEL_WIDTH ** -0.5, 0.0625, ((0, 32), (1, 8)))
    k_cache = draw_k_cache(jax.random.fold_in(streams_of[11], 71), 0)
    value_cache = normal_values(streams_of[4], (KEY_VALUE_HEADS, N_KVP * SLOTS_PER_SPLIT, PAGE_TOKENS, HEAD_WIDTH), 8.0, 48.0, ((0, 8), (1, 32)))
    page_table = draw_page_table(jax.random.fold_in(streams_of[11], 71), 0)
    lengths = draw_lengths(jax.random.fold_in(streams_of[11], 71), 0)
    output_weight = normal_values(streams_of[7], (KEY_VALUE_HEADS, QUERY_PER_KEY * HEAD_WIDTH, MODEL_WIDTH), (QUERY_PER_KEY * HEAD_WIDTH) ** -0.5, 0.1875, ((0, 8), (2, 32)))
    mlp_gain = jnp.clip(1.0 + 0.18 * jax.random.normal(streams_of[8], (MODEL_WIDTH,), jnp.float32), 0.099609375, 1.8984375).astype(jnp.bfloat16)
    w_in = normal_values(streams_of[9], (MODEL_WIDTH, 2, FF), MODEL_WIDTH ** -0.5, 0.0625, ((0, 32), (2, 8)))
    w_down = normal_values(streams_of[10], (FF, MODEL_WIDTH), (FF // 16) ** -0.5, 0.15625, ((0, 8), (1, 32)))
    return {"hidden_in": hidden_in, "attn_gain": attn_gain, "query_key_value_weight": query_key_value_weight, "k_cache": k_cache, "value_cache": value_cache, "page_table": page_table, "lengths": lengths, "output_weight": output_weight, "mlp_gain": mlp_gain, "w_in": w_in, "w_down": w_down}


EPSILON = 1e-05
ROPE_BASE = 10000.0

def rotate(vector, position):
    half_size = vector.shape[-1] // 2
    exponent = jnp.arange(half_size, dtype=jnp.float32) * (2.0 / vector.shape[-1])
    inverse = ROPE_BASE ** (-exponent)
    angles = position.astype(jnp.float32)[:, None] * inverse[None, :]
    target_shape = (angles.shape[0],) + (1,) * (vector.ndim - 2) + (half_size,)
    cosine = jnp.cos(angles).reshape(target_shape)
    sine_part = jnp.sin(angles).reshape(target_shape)
    front_half = vector[..., :half_size]
    back_half = vector[..., half_size:]
    return jnp.concatenate([front_half * cosine - back_half * sine_part, back_half * cosine + front_half * sine_part], axis=-1)

def reference(hidden_in, attn_gain, query_key_value_weight, k_cache, value_cache, page_table, lengths, output_weight, mlp_gain, w_in, w_down):
    stream = hidden_in.astype(jnp.float32)
    normed = (stream * attn_gain.astype(jnp.float32)).astype(jnp.bfloat16)
    attention_scale = lax.rsqrt(lax.optimization_barrier(jnp.mean(stream * stream, axis=1)) + EPSILON)
    projected_rows = jnp.dot(normed, query_key_value_weight.reshape(MODEL_WIDTH, -1), preferred_element_type=jnp.float32)
    projected_rows = (projected_rows * attention_scale[:, None]).reshape(REQUEST_COUNT, KEY_VALUE_HEADS, QUERY_PER_KEY + 2, HEAD_WIDTH)
    queries = rotate(projected_rows[:, :, :QUERY_PER_KEY, :], lengths).astype(jnp.bfloat16)
    new_keys = rotate(projected_rows[:, :, QUERY_PER_KEY, :], lengths).astype(jnp.bfloat16)
    new_values = projected_rows[:, :, QUERY_PER_KEY + 1, :].astype(jnp.bfloat16)
    shard_of_page = jnp.arange(PAGES, dtype=jnp.int32) // PAGES_DEV
    slot_rows = (page_table + (shard_of_page * SLOTS_PER_SPLIT)[None, :]).astype(jnp.int32)
    live_mask = jnp.arange(CTX, dtype=jnp.int32)[None, :] < lengths[:, None]
    factor = HEAD_WIDTH ** (-0.5)

    def one_head(inputs):
        key_pool, value_pool, head_queries, head_key, head_value = inputs
        cached_keys = key_pool[slot_rows].reshape(REQUEST_COUNT, CTX, HEAD_WIDTH).astype(jnp.float32)
        cached_values = value_pool[slot_rows].reshape(REQUEST_COUNT, CTX, HEAD_WIDTH).astype(jnp.float32)
        query_float = head_queries.astype(jnp.float32)
        scores = jnp.einsum('bgd,bcd->bgc', query_float, cached_keys) * factor
        scores = jnp.where(live_mask[:, None, :], scores, -1e+30)
        own = lax.optimization_barrier(jnp.sum(query_float * head_key.astype(jnp.float32)[:, None, :], axis=-1)) * factor
        maxima = jnp.maximum(lax.optimization_barrier(jnp.max(scores, axis=-1)), own)
        weights = jnp.exp(scores - maxima[..., None])
        own_weight = jnp.exp(own - maxima)
        totals = lax.optimization_barrier(jnp.sum(weights, axis=-1)) + own_weight
        rounded = lax.optimization_barrier(weights.astype(jnp.bfloat16)).astype(jnp.float32)
        own_rounded = lax.optimization_barrier(own_weight.astype(jnp.bfloat16)).astype(jnp.float32)
        summed = jnp.einsum('bgc,bcd->bgd', rounded, cached_values)
        summed = summed + own_rounded[..., None] * head_value.astype(jnp.float32)[:, None, :]
        return (summed / totals[..., None]).astype(jnp.bfloat16)
    attn = lax.map(one_head, (k_cache, value_cache, jnp.transpose(queries, (1, 0, 2, 3)), jnp.transpose(new_keys, (1, 0, 2)), jnp.transpose(new_values, (1, 0, 2))))
    attn = jnp.transpose(attn, (1, 0, 2, 3)).reshape(REQUEST_COUNT, -1)
    stream = stream + jnp.dot(attn, output_weight.reshape(-1, MODEL_WIDTH), preferred_element_type=jnp.float32)
    normed_mlp = (stream * mlp_gain.astype(jnp.float32)).astype(jnp.bfloat16)
    scale_mlp = lax.rsqrt(lax.optimization_barrier(jnp.mean(stream * stream, axis=1)) + EPSILON)
    both_parts = jnp.dot(normed_mlp, w_in.reshape(MODEL_WIDTH, -1), preferred_element_type=jnp.float32)
    both_parts = both_parts.reshape(REQUEST_COUNT, 2, FF) * scale_mlp[:, None, None]
    hidden = (jax.nn.silu(both_parts[:, 0]) * both_parts[:, 1]).astype(jnp.bfloat16)
    result = stream + jnp.dot(hidden, w_down, preferred_element_type=jnp.float32)
    return result.astype(jnp.bfloat16)
```

```python
import functools
import math

import jax
import jax.numpy as jnp
import numpy as np
from jax import lax
from jax.experimental import pallas as pl
from jax.experimental.pallas import tpu as pltpu
from jax.sharding import PartitionSpec as P

MESH = pl.DeviceIdType.MESH
F32 = jnp.float32
BF16 = jnp.bfloat16

MODEL_WIDTH = 8192
EPSILON = 1e-05
ROPE_BASE = 10000.0
B = 16
G = 8
D = 128
N = 32
H = 8
PAGE = 128
PAGES_HERE = 4
TILES_QKV = G + 2
LANES = 128

SPREAD, UNSPREAD = 5, 13


def iota(shape, dim):
    return lax.broadcasted_iota(jnp.int32, shape, dim)


def to_row(column):
    wide = jnp.broadcast_to(column, (B, LANES))
    kept = jnp.where(iota((B, LANES), 0) == iota((B, LANES), 1), wide, 0.0)
    return jnp.sum(kept, axis=0, keepdims=True)


def to_column(row):
    wide = jnp.broadcast_to(row, (B, LANES))
    kept = jnp.where(iota((B, LANES), 0) == iota((B, LANES), 1), wide, 0.0)
    return jnp.sum(kept, axis=1, keepdims=True)


def sine_and_cosine(angle):
    turns = jnp.floor(angle * (1.0 / (2.0 * math.pi)) + 0.5)
    left = angle - turns * 6.28125
    left = left - turns * (2.0 * math.pi - 6.28125)
    y = left * 0.5
    z = y * y
    sine, cosine = 0.0, 0.0
    for k in range(6, -1, -1):
        sine = sine * z + (-1.0) ** k / math.factorial(2 * k + 1)
    for k in range(7, -1, -1):
        cosine = cosine * z + (-1.0) ** k / math.factorial(2 * k)
    sine = sine * y
    return 2.0 * sine * cosine, 1.0 - 2.0 * sine * sine


def kernel(
    tiles_ff,
    ff,
    hidden_hbm,
    attn_gain_ref,
    qkv_hbm,
    k_hbm,
    v_hbm,
    table_ref,
    lengths_ref,
    wo_hbm,
    mlp_gain_ref,
    win_hbm,
    wdown_hbm,
    inverse_ref,
    out_ref,
    hidden,
    wqkv,
    keys,
    values,
    wo,
    win,
    wdown,
    qkv_send,
    qkv_recv,
    square_send,
    square_recv,
    q_all,
    q_rows,
    part_send,
    part_recv,
    attn_all,
    attn_rows,
    head_send,
    head_recv,
    ff_send,
    ff_recv,
    square2_send,
    square2_recv,
    hid_all,
    last_send,
    last_recv,
    local_sem,
    send_sem,
    recv_sem,
):
    me = lax.axis_index("kvp")
    my_head = lax.axis_index("head")
    mine = lax.rem(me * UNSPREAD, N)

    def copy_to(src, dst, phase, device):
        pltpu.make_async_remote_copy(
            src_ref=src,
            dst_ref=dst,
            send_sem=send_sem.at[phase],
            recv_sem=recv_sem.at[phase],
            device_id=device,
            device_id_type=MESH,
        ).start()

    def waiter(ref, phase):
        return pltpu.make_async_remote_copy(
            src_ref=ref,
            dst_ref=ref,
            send_sem=send_sem.at[phase],
            recv_sem=recv_sem.at[phase],
            device_id={"kvp": lax.rem(me + 1, N)},
            device_id_type=MESH,
        )

    def loads():
        yield hidden_hbm, hidden
        yield qkv_hbm, wqkv
        yield k_hbm.at[pl.ds(0, 32)], keys.at[pl.ds(0, 32)]
        yield k_hbm.at[pl.ds(32, 32)], keys.at[pl.ds(32, 32)]
        yield v_hbm.at[pl.ds(0, 32)], values.at[pl.ds(0, 32)]
        yield v_hbm.at[pl.ds(32, 32)], values.at[pl.ds(32, 32)]
        yield wo_hbm, wo
        yield win_hbm.at[0], win.at[0, pl.ds(0, ff)]
        yield win_hbm.at[1], win.at[1, pl.ds(0, ff)]
        yield wdown_hbm, wdown.at[pl.ds(0, ff)]

    copies = [
        pltpu.make_async_copy(src, dst, local_sem.at[at]) for at, (src, dst) in enumerate(loads())
    ]
    for copy in copies:
        copy.start()

    barrier = pltpu.get_barrier_semaphore()

    @pl.loop(1, N)
    def _(step):
        pl.semaphore_signal(
            barrier, inc=1, device_id={"kvp": lax.rem(me + step, N)}, device_id_type=MESH
        )

    @pl.loop(1, H)
    def _(step):
        pl.semaphore_signal(
            barrier, inc=1, device_id={"head": lax.rem(my_head + step, H)}, device_id_type=MESH
        )

    pad = win.shape[1] - ff
    win[:, pl.ds(ff, pad), :] = jnp.zeros((2, pad, win.shape[2]), BF16)
    wdown[pl.ds(ff, pad), :] = jnp.zeros((pad, wdown.shape[1]), BF16)

    rows = iota((B, LANES), 0)
    position = jnp.zeros((B, LANES), F32)
    for b in range(B):
        position = jnp.where(rows == b, lengths_ref[b].astype(F32), position)
    sine, cosine = sine_and_cosine(position * inverse_ref[0:1, :])
    sine = jnp.where(iota((B, LANES), 1) < D // 2, -sine, sine)

    copies[0].wait()
    copies[1].wait()
    x = hidden[...].astype(F32)
    normed = (x * attn_gain_ref[...][None, :].astype(F32)).astype(BF16)
    partial = jnp.dot(normed, wqkv[...], preferred_element_type=F32).astype(BF16)
    for t in range(TILES_QKV):
        qkv_send[t] = partial[:, t * D : (t + 1) * D]
    square_row = to_row(jnp.sum(x * x, axis=1, keepdims=True))
    square_send[...] = square_row

    pl.semaphore_wait(barrier, N - 1 + H - 1)

    def scatter(tiles, send):
        @pl.loop(1, N)
        def _(step):
            t = lax.rem(mine + step, N)

            @pl.when(t < tiles)
            def _():
                send(t, {"kvp": lax.rem(t * SPREAD, N)})

    def spread(all_ref, phase):
        @pl.loop(1, N)
        def _(step):
            copy_to(
                all_ref.at[mine], all_ref.at[mine], phase, {"kvp": lax.rem(me + step, N)}
            )

    def wait_gathered(all_ref, tiles, phase):
        @pl.when(mine < tiles)
        def _():
            waiter(all_ref.at[pl.ds(0, tiles - 1)], phase).wait_recv()

        @pl.when(mine >= tiles)
        def _():
            waiter(all_ref, phase).wait_recv()

    def send_qkv(t, device):
        copy_to(qkv_send.at[t], qkv_recv.at[me], 0, device)
        copy_to(square_send, square_recv.at[me], 1, device)

    scatter(TILES_QKV, send_qkv)

    @pl.when(mine < TILES_QKV)
    def _():
        qkv_recv[me] = qkv_send[mine]
        square_recv[me] = square_row
        waiter(square_recv.at[pl.ds(0, N - 1)], 1).wait_recv()
        waiter(qkv_recv.at[pl.ds(0, N - 1)], 0).wait_recv()
        square = to_column(jnp.sum(square_recv[...], axis=0))
        scale = lax.rsqrt(square / MODEL_WIDTH + EPSILON)
        total = jnp.sum(qkv_recv[...].astype(F32), axis=0) * scale
        turned = total * cosine + pltpu.roll(total, D // 2, 1) * sine
        q_all[mine] = jnp.where(mine < G + 1, turned, total).astype(BF16)
        spread(q_all, 2)

    for copy in copies[2:6]:
        copy.wait()
    wait_gathered(q_all, TILES_QKV, 2)

    q_rows[...] = q_all[...].astype(F32).reshape(TILES_QKV * B, D)
    factor = D ** (-0.5)
    lane = iota((G, LANES), 1)
    first = me * (PAGES_HERE * PAGE)
    for b in range(B):
        query = q_rows[pl.ds(b, G, stride=B), :].astype(BF16)
        left = lengths_ref[b] - first
        slots = [table_ref[p, b] for p in range(PAGES_HERE)]
        scores, live = [], []
        for p in range(PAGES_HERE):
            score = lax.dot_general(
                query, keys[slots[p]], (((1,), (1,)), ((), ())), preferred_element_type=F32
            )
            live.append(lane + p * PAGE < left)
            scores.append(jnp.where(live[p], score * factor, -1e30))
        top = functools.reduce(jnp.maximum, scores)
        top = jnp.max(top, axis=1, keepdims=True)
        weights = [jnp.where(ok, jnp.exp(s - top), 0.0) for ok, s in zip(live, scores)]
        total = jnp.sum(functools.reduce(jnp.add, weights), axis=1, keepdims=True)
        summed = 0.0
        for p in range(PAGES_HERE):
            summed = summed + jnp.dot(
                weights[p].astype(BF16), values[slots[p]], preferred_element_type=F32
            )
        high = top.astype(BF16).astype(F32)
        middle = (top - high).astype(BF16).astype(F32)
        low = top - high - middle
        stats = jnp.where(
            lane < 32, high, jnp.where(lane < 64, middle, jnp.where(lane < 96, low, total))
        )
        part_send[b] = jnp.concatenate([summed, stats], axis=0).astype(BF16)

    def send_part(t, device):
        copy_to(part_send.at[t], part_recv.at[me], 3, device)

    scatter(B, send_part)

    @pl.when(mine < B)
    def _():
        query = q_rows[pl.ds(mine, G, stride=B), :]
        new_key = q_rows[pl.ds(G * B + mine, 1), :]
        new_value = q_rows[pl.ds((G + 1) * B + mine, 1), :]
        own = jnp.sum(query * new_key, axis=1, keepdims=True) * factor
        part_recv[me] = part_send[mine]
        waiter(part_recv.at[pl.ds(0, N - 1)], 3).wait_recv()
        tops, overall = [], own
        for k in range(N):
            stats = part_recv[k].astype(F32)[G:]
            tops.append(stats[:, 0:1] + stats[:, 32:33] + stats[:, 64:65])
            overall = jnp.maximum(overall, tops[k])
        own_weight = jnp.exp(own - overall)
        total = own_weight
        summed = own_weight.astype(BF16).astype(F32) * new_value
        for k in range(N):
            tile = part_recv[k].astype(F32)
            carried = jnp.exp(tops[k] - overall)
            total = total + tile[G:, 96:97] * carried
            summed = summed + tile[:G] * carried
        attn_all[mine] = (summed / total).astype(BF16)
        spread(attn_all, 4)

    copies[6].wait()
    wait_gathered(attn_all, B, 4)

    attn_rows[...] = attn_all[...].astype(F32).reshape(B * G, D)
    attn = jnp.concatenate(
        [attn_rows[pl.ds(g, B, stride=G), :].astype(BF16) for g in range(G)], axis=1
    )

    def over_heads(term, send_ref, recv_ref, phase):
        send_ref[...] = term.astype(BF16)
        recv_ref[my_head] = term.astype(BF16)

        @pl.loop(1, H)
        def _(step):
            copy_to(
                send_ref, recv_ref.at[my_head], phase, {"head": lax.rem(my_head + step, H)}
            )

        waiter(recv_ref.at[pl.ds(0, H - 1)], phase).wait_recv()
        return jnp.sum(recv_ref[...].astype(F32), axis=0)

    term = jnp.dot(attn, wo[...], preferred_element_type=F32)
    stream = x + over_heads(term, head_send, head_recv, 5)

    square2_row = to_row(jnp.sum(stream * stream, axis=1, keepdims=True))
    square2_send[...] = square2_row
    normed = (stream * mlp_gain_ref[...][None, :].astype(F32)).astype(BF16)
    copies[7].wait()
    copies[8].wait()
    for t in range(tiles_ff):
        for part in range(2):
            ff_send[t, part] = lax.dot_general(
                normed,
                win[part, pl.ds(t * LANES, LANES), :],
                (((1,), (1,)), ((), ())),
                preferred_element_type=F32,
            ).astype(BF16)

    def send_ff(t, device):
        copy_to(ff_send.at[t], ff_recv.at[me], 6, device)
        copy_to(square2_send, square2_recv.at[me], 7, device)

    scatter(tiles_ff, send_ff)

    @pl.when(mine < tiles_ff)
    def _():
        ff_recv[me] = ff_send[mine]
        square2_recv[me] = square2_row
        waiter(square2_recv.at[pl.ds(0, N - 1)], 7).wait_recv()
        waiter(ff_recv.at[pl.ds(0, N - 1)], 6).wait_recv()
        square = to_column(jnp.sum(square2_recv[...], axis=0))
        scale = lax.rsqrt(square / MODEL_WIDTH + EPSILON)
        both = jnp.sum(ff_recv[...].astype(F32), axis=0)
        gate, up = both[0] * scale, both[1] * scale
        hid_all[mine] = (gate / (1.0 + jnp.exp(-gate)) * up).astype(BF16)
        spread(hid_all, 8)

    copies[9].wait()
    wait_gathered(hid_all, tiles_ff, 8)

    active = jnp.concatenate([hid_all[t] for t in range(tiles_ff)], axis=1)
    term = jnp.dot(active, wdown[...], preferred_element_type=F32)
    out_ref[...] = (stream + over_heads(term, last_send, last_recv, 9)).astype(BF16)

    def wait_scattered(recv_ref, tiles, phase):
        @pl.when(mine < tiles)
        def _():
            waiter(recv_ref.at[pl.ds(0, tiles - 1)], phase).wait_send()

        @pl.when(mine >= tiles)
        def _():
            waiter(recv_ref.at[pl.ds(0, tiles)], phase).wait_send()

    wait_scattered(qkv_recv, TILES_QKV, 0)
    wait_scattered(square_recv, TILES_QKV, 1)
    wait_scattered(part_recv, B, 3)
    wait_scattered(ff_recv, tiles_ff, 6)
    wait_scattered(square2_recv, tiles_ff, 7)

    @pl.when(mine < TILES_QKV)
    def _():
        waiter(qkv_recv.at[pl.ds(0, N - 1)], 2).wait_send()

    @pl.when(mine < B)
    def _():
        waiter(part_recv.at[pl.ds(0, N - 1), pl.ds(0, G)], 4).wait_send()

    @pl.when(mine < tiles_ff)
    def _():
        waiter(part_recv.at[pl.ds(0, N - 1)], 8).wait_send()

    waiter(head_recv.at[pl.ds(0, H - 1)], 5).wait_send()
    waiter(last_recv.at[pl.ds(0, H - 1)], 9).wait_send()


def on_device(
    hidden_in,
    attn_gain,
    query_key_value_weight,
    k_cache,
    value_cache,
    page_table,
    lengths,
    output_weight,
    mlp_gain,
    w_in,
    w_down,
):
    width = hidden_in.shape[1]
    ff = w_down.shape[0]
    tiles_ff = -(-ff // LANES)
    half = D // 2
    inverse = ROPE_BASE ** (-np.arange(half, dtype=np.float64) * (2.0 / D))
    inverse = np.broadcast_to(np.concatenate([inverse, inverse]), (8, D)).astype(np.float32)
    any_space = pl.BlockSpec(memory_space=pl.ANY)
    vmem = pl.BlockSpec(memory_space=pltpu.VMEM)
    smem = pl.BlockSpec(memory_space=pltpu.SMEM)
    slots = k_cache.shape[1]
    return pl.pallas_call(
        functools.partial(kernel, tiles_ff, ff),
        out_shape=jax.ShapeDtypeStruct((B, width), BF16),
        in_specs=[
            any_space,
            vmem,
            any_space,
            any_space,
            any_space,
            smem,
            smem,
            any_space,
            vmem,
            any_space,
            any_space,
            vmem,
        ],
        out_specs=vmem,
        scratch_shapes=[
            pltpu.VMEM((B, width), BF16),
            pltpu.VMEM((width, TILES_QKV * D), BF16),
            pltpu.VMEM((slots, PAGE, D), BF16),
            pltpu.VMEM((slots, PAGE, D), BF16),
            pltpu.VMEM((G * D, width), BF16),
            pltpu.VMEM((2, tiles_ff * LANES, width), BF16),
            pltpu.VMEM((tiles_ff * LANES, width), BF16),
            pltpu.VMEM((TILES_QKV, B, D), BF16),
            pltpu.VMEM((N, B, D), BF16),
            pltpu.VMEM((1, LANES), F32),
            pltpu.VMEM((N, 1, LANES), F32),
            pltpu.VMEM((TILES_QKV, B, D), BF16),
            pltpu.VMEM((TILES_QKV * B, D), F32),
            pltpu.VMEM((B, 2 * G, D), BF16),
            pltpu.VMEM((N, 2 * G, D), BF16),
            pltpu.VMEM((B, G, D), BF16),
            pltpu.VMEM((B * G, D), F32),
            pltpu.VMEM((B, width), BF16),
            pltpu.VMEM((H, B, width), BF16),
            pltpu.VMEM((tiles_ff, 2, B, LANES), BF16),
            pltpu.VMEM((N, 2, B, LANES), BF16),
            pltpu.VMEM((1, LANES), F32),
            pltpu.VMEM((N, 1, LANES), F32),
            pltpu.VMEM((tiles_ff, B, LANES), BF16),
            pltpu.VMEM((B, width), BF16),
            pltpu.VMEM((H, B, width), BF16),
            pltpu.SemaphoreType.DMA((10,)),
            pltpu.SemaphoreType.DMA((10,)),
            pltpu.SemaphoreType.DMA((10,)),
        ],
        compiler_params=pltpu.CompilerParams(collective_id=0, has_side_effects=True),
    )(
        hidden_in,
        attn_gain,
        query_key_value_weight.transpose(1, 0, 2)[0],
        k_cache[0],
        value_cache[0],
        page_table.T,
        lengths,
        output_weight[0],
        mlp_gain,
        w_in.transpose(1, 2, 0),
        w_down,
        jnp.asarray(inverse),
    )


def solution(mesh):
    return jax.shard_map(
        on_device,
        mesh=mesh,
        in_specs=(
            P(None, "kvp"),
            P("kvp"),
            P("kvp", "head", None),
            P("head", "kvp", None, None),
            P("head", "kvp", None, None),
            P(None, "kvp"),
            P(),
            P("head", None, "kvp"),
            P("kvp"),
            P("kvp", None, "head"),
            P("head", "kvp"),
        ),
        out_specs=P(None, "kvp"),
        check_vma=False,
    )
```

```python
import functools
import math

import jax
import jax.numpy as jnp
import numpy as np
from jax import lax
from jax.experimental import pallas as pl
from jax.experimental.pallas import tpu as pltpu
from jax.sharding import PartitionSpec as P

MESH = pl.DeviceIdType.MESH
F32 = jnp.float32
BF16 = jnp.bfloat16

MODEL_WIDTH = 8192
EPSILON = 1e-05
ROPE_BASE = 10000.0
B = 16
G = 8
D = 128
Z, X = 8, 4
N = Z * X
Y, C = 4, 2
H = Y * C
PAGE = 128
PAGES_HERE = 4
VECTORS = G + 2
LANES = 128
SQUARE_ROW = VECTORS
GROUP = 8


def around(offset, size):
    return min(offset % size, -offset % size)


def far_first(offsets, sizes):
    return sorted(offsets, key=lambda at: -sum(around(o, s) for o, s in zip(at, sizes)))


ALL = far_first([(dz, dx) for dz in range(Z) for dx in range(X) if (dz, dx) != (0, 0)], (Z, X))
NEAR = far_first(
    [(dz, dx) for dz in (-1, 0, 1, 2) for dx in range(X) if (dz, dx) != (0, 0)], (Z, X)
)
HEADS = far_first([(dy, dc) for dy in range(Y) for dc in range(C) if (dy, dc) != (0, 0)], (Y, C))


def iota(shape, dim):
    return lax.broadcasted_iota(jnp.int32, shape, dim)


def to_row(column):
    wide = jnp.broadcast_to(column, (B, LANES))
    kept = jnp.where(iota((B, LANES), 0) == iota((B, LANES), 1), wide, 0.0)
    return jnp.sum(kept, axis=0, keepdims=True)


def to_column(row):
    wide = jnp.broadcast_to(row, (B, LANES))
    kept = jnp.where(iota((B, LANES), 0) == iota((B, LANES), 1), wide, 0.0)
    return jnp.sum(kept, axis=1, keepdims=True)


def rounded(value):
    return value.astype(BF16).astype(F32)


def sine_and_cosine(angle):
    turns = jnp.floor(angle * (1.0 / (2.0 * math.pi)) + 0.5)
    left = angle - turns * 6.28125
    left = left - turns * (2.0 * math.pi - 6.28125)
    y = left * 0.5
    z = y * y
    sine, cosine = 0.0, 0.0
    for k in range(6, -1, -1):
        sine = sine * z + (-1.0) ** k / math.factorial(2 * k + 1)
    sine = sine * y
    for k in range(7, -1, -1):
        cosine = cosine * z + (-1.0) ** k / math.factorial(2 * k)
    return 2.0 * sine * cosine, 1.0 - 2.0 * sine * sine


def kernel(
    tiles_ff,
    ff,
    hidden_hbm,
    attn_gain_hbm,
    qkv_hbm,
    k_hbm,
    v_hbm,
    table_hbm,
    lengths_hbm,
    wo_hbm,
    mlp_gain_hbm,
    win_hbm,
    wdown_hbm,
    inverse_hbm,
    out_ref,
    hidden,
    attn_gain,
    mlp_gain,
    inverse,
    table,
    lengths,
    wqkv,
    keys,
    values,
    wo,
    win,
    wdown,
    turned,
    qkv_send,
    qkv_recv,
    q_all,
    part_send,
    part_recv,
    attn_all,
    attn_rows,
    head_send,
    head_recv,
    ff_send,
    ff_recv,
    square_send,
    square_recv,
    hid_all,
    last_send,
    last_recv,
    local_sem,
    send_sem,
    recv_sem,
):
    me = lax.axis_index("kvp")
    my_head = lax.axis_index("head")
    my_z, my_x = me // X, lax.rem(me, X)
    my_y, my_c = my_head // C, lax.rem(my_head, C)
    zs = [lax.rem(my_z + dz, Z) for dz in range(Z)]
    xs = [lax.rem(my_x + dx, X) for dx in range(X)]
    ys = [lax.rem(my_y + dy, Y) for dy in range(Y)]
    cs = [lax.rem(my_c + dc, C) for dc in range(C)]

    def peer(dz, dx):
        return {"kvp": zs[dz % Z] * X + xs[dx % X]}

    def head_peer(dy, dc):
        return {"head": ys[dy] * C + cs[dc]}

    request_of_z = [lax.rem(z, Z // 2) * X for z in zs]
    tile_of_z = [lax.rem(z * 20, N) for z in zs]
    tile_of_x = [x * 13 for x in xs]

    def request_at(dz, dx):
        return request_of_z[dz % Z] + xs[dx % X]

    def tile_at(dz, dx):
        return lax.rem(tile_of_z[dz % Z] + tile_of_x[dx % X], N)

    my_request = request_at(0, 0)
    my_tile = tile_at(0, 0)

    def copy_to(src, dst, phase, device):
        pltpu.make_async_remote_copy(
            src_ref=src,
            dst_ref=dst,
            send_sem=send_sem.at[phase],
            recv_sem=recv_sem.at[phase],
            device_id=device,
            device_id_type=MESH,
        ).start()

    def waiter(ref, phase):
        return pltpu.make_async_remote_copy(
            src_ref=ref,
            dst_ref=ref,
            send_sem=send_sem.at[phase],
            recv_sem=recv_sem.at[phase],
            device_id=peer(1, 0),
            device_id_type=MESH,
        )

    barrier = pltpu.get_barrier_semaphore()
    for offset in ALL:
        pl.semaphore_signal(barrier, inc=1, device_id=peer(*offset), device_id_type=MESH)
    for offset in HEADS:
        pl.semaphore_signal(barrier, inc=1, device_id=head_peer(*offset), device_id_type=MESH)

    pairs = [
        (hidden_hbm, hidden),
        (attn_gain_hbm, attn_gain),
        (qkv_hbm, wqkv),
        (lengths_hbm, lengths),
        (inverse_hbm, inverse),
        (table_hbm, table),
        (k_hbm.at[pl.ds(0, 32)], keys.at[pl.ds(0, 32)]),
        (k_hbm.at[pl.ds(32, 32)], keys.at[pl.ds(32, 32)]),
        (v_hbm.at[pl.ds(0, 32)], values.at[pl.ds(0, 32)]),
        (v_hbm.at[pl.ds(32, 32)], values.at[pl.ds(32, 32)]),
        (wo_hbm, wo),
        (mlp_gain_hbm, mlp_gain),
        (win_hbm.at[0], win.at[0, pl.ds(0, ff)]),
        (win_hbm.at[1], win.at[1, pl.ds(0, ff)]),
        (wdown_hbm, wdown.at[pl.ds(0, ff)]),
    ]
    copies = [
        pltpu.make_async_copy(src, dst, local_sem.at[at]) for at, (src, dst) in enumerate(pairs)
    ]
    for copy in copies:
        copy.start()

    pad = win.shape[1] - ff
    win[:, pl.ds(ff, pad), :] = jnp.zeros((2, pad, win.shape[2]), BF16)
    wdown[pl.ds(ff, pad), :] = jnp.zeros((pad, wdown.shape[1]), BF16)
    turned[...] = jnp.zeros(turned.shape, F32)

    for copy in copies[:3]:
        copy.wait()
    x = hidden[...].astype(F32)
    normed = (x * attn_gain[...][None, :].astype(F32)).astype(BF16)
    partial = jnp.dot(normed, wqkv[...], preferred_element_type=F32)
    for v in range(VECTORS):
        turned[pl.ds(v, B, stride=2 * G), :] = partial[:, v * D : (v + 1) * D]
    square = jnp.sum(x * x, axis=1, keepdims=True)
    high = rounded(square)
    turned[pl.ds(SQUARE_ROW, B, stride=2 * G), :] = jnp.where(
        iota((B, LANES), 1) < LANES // 2, high, square - high
    )
    qkv_send[...] = turned[...].reshape(B, 2 * G, D).astype(BF16)
    qkv_recv[me] = qkv_send[my_request]

    pl.semaphore_wait(barrier, len(ALL) + len(HEADS))

    for offset in ALL:
        copy_to(qkv_send.at[request_at(*offset)], qkv_recv.at[me], 0, peer(*offset))
    for copy in copies[3:6]:
        copy.wait()
    sine, cosine = sine_and_cosine(lengths[my_request].astype(F32) * inverse[...])
    lane = iota((G, LANES), 1)
    sine = jnp.where(lane < D // 2, -sine, sine)[0:1]
    cosine = cosine[0:1]
    for copy in copies[6:10]:
        copy.wait()
    waiter(qkv_recv.at[pl.ds(0, len(ALL))], 0).wait_recv()
    total = jnp.sum(qkv_recv[...].astype(F32), axis=0)
    square = total[SQUARE_ROW : SQUARE_ROW + 1]
    square = square[:, 0:1] + square[:, LANES // 2 : LANES // 2 + 1]
    total = total * lax.rsqrt(square / MODEL_WIDTH + EPSILON)
    rotated = total * cosine + pltpu.roll(total, D // 2, 1) * sine
    q_all[my_request] = rotated[:G].astype(BF16)
    for offset in NEAR:
        copy_to(q_all.at[my_request], q_all.at[my_request], 1, peer(*offset))
    factor = D ** (-0.5)
    new_key, new_value = rounded(rotated[G : G + 1]), rounded(total[G + 1 : G + 2])
    own = jnp.sum(rounded(rotated[:G]) * new_key, axis=1, keepdims=True) * factor
    waiter(q_all.at[pl.ds(0, len(NEAR))], 1).wait_recv()

    first = me * (PAGES_HERE * PAGE)
    slots = [[table[p, b] for p in range(PAGES_HERE)] for b in range(B)]
    scores = [
        [
            lax.dot_general(
                q_all[b], keys[slot], (((1,), (1,)), ((), ())), preferred_element_type=F32
            )
            for slot in slots[b]
        ]
        for b in range(B)
    ]
    parts = []
    for b in range(B):
        left = lengths[b] - first
        live = [lane + p * PAGE < left for p in range(PAGES_HERE)]
        masked = [jnp.where(ok, s * factor, -1e30) for ok, s in zip(live, scores[b])]
        top = jnp.max(functools.reduce(jnp.maximum, masked), axis=1, keepdims=True)
        weights = [jnp.where(ok, jnp.exp(s - top), 0.0) for ok, s in zip(live, masked)]
        total = jnp.sum(functools.reduce(jnp.add, weights), axis=1, keepdims=True)
        summed = 0.0
        for p in range(PAGES_HERE):
            summed = summed + jnp.dot(
                weights[p].astype(BF16), values[slots[b][p]], preferred_element_type=F32
            )
        high = rounded(top)
        middle = rounded(top - high)
        low = top - high - middle
        stats = jnp.where(
            lane < 32, high, jnp.where(lane < 64, middle, jnp.where(lane < 96, low, total))
        )
        parts.append(jnp.concatenate([summed, stats], axis=0).astype(BF16))
    for b in range(B):
        part_send[b] = parts[b]

    for offset in ALL:
        copy_to(part_send.at[request_at(*offset)], part_recv.at[me], 2, peer(*offset))
    part_recv[me] = part_send[my_request]
    copies[10].wait()
    waiter(part_recv.at[pl.ds(0, len(ALL))], 2).wait_recv()
    tops, overall = [], own
    for k in range(N):
        stats = part_recv[k].astype(F32)[G:]
        tops.append(stats[:, 0:1] + stats[:, 32:33] + stats[:, 64:65])
        overall = jnp.maximum(overall, tops[k])
    own_weight = jnp.exp(own - overall)
    total = own_weight
    summed = rounded(own_weight) * new_value
    for k in range(N):
        tile = part_recv[k].astype(F32)
        carried = jnp.exp(tops[k] - overall)
        total = total + tile[G:, 96:97] * carried
        summed = summed + tile[:G] * carried
    attn_all[my_request] = (summed / total).astype(BF16)
    for offset in NEAR:
        copy_to(attn_all.at[my_request], attn_all.at[my_request], 3, peer(*offset))
    waiter(attn_all.at[pl.ds(0, len(NEAR))], 3).wait_recv()

    attn_rows[...] = attn_all[...].astype(F32).reshape(B * G, D)
    attn = jnp.concatenate(
        [attn_rows[pl.ds(g, B, stride=G), :].astype(BF16) for g in range(G)], axis=1
    )

    def over_heads(term, send_ref, recv_ref, phase):
        send_ref[...] = term.astype(BF16)
        for offset in HEADS:
            copy_to(send_ref, recv_ref.at[my_head], phase, head_peer(*offset))
        recv_ref[my_head] = term.astype(BF16)
        waiter(recv_ref.at[pl.ds(0, len(HEADS))], phase).wait_recv()
        return jnp.sum(recv_ref[...].astype(F32), axis=0)

    term = jnp.dot(attn, wo[...], preferred_element_type=F32)
    for copy in copies[11:14]:
        copy.wait()
    stream = x + over_heads(term, head_send, head_recv, 4)

    square_row = to_row(jnp.sum(stream * stream, axis=1, keepdims=True))
    square_send[...] = square_row
    normed = (stream * mlp_gain[...][None, :].astype(F32)).astype(BF16)
    for start in range(0, N, GROUP):
        group = (ALL + [(0, 0)])[start : start + GROUP]
        for offset in group:
            tile = tile_at(*offset)
            rows = pl.ds(pl.multiple_of(jnp.minimum(tile, tiles_ff - 1) * LANES, LANES), LANES)
            for part in range(2):
                ff_send[tile, part] = lax.dot_general(
                    normed,
                    win[part, rows, :],
                    (((1,), (1,)), ((), ())),
                    preferred_element_type=F32,
                ).astype(BF16)
        for offset in group:
            if offset != (0, 0):
                tile = tile_at(*offset)

                @pl.when(tile < tiles_ff)
                def _(tile=tile, offset=offset):
                    copy_to(ff_send.at[tile], ff_recv.at[me], 5, peer(*offset))
                    copy_to(square_send, square_recv.at[me], 6, peer(*offset))

    @pl.when(my_tile < tiles_ff)
    def _():
        ff_recv[me] = ff_send[my_tile]
        square_recv[me] = square_row
        waiter(square_recv.at[pl.ds(0, N - 1)], 6).wait_recv()
        waiter(ff_recv.at[pl.ds(0, N - 1)], 5).wait_recv()
        square = to_column(jnp.sum(square_recv[...], axis=0))
        scale = lax.rsqrt(square / MODEL_WIDTH + EPSILON)
        both = jnp.sum(ff_recv[...].astype(F32), axis=0)
        gate, up = both[0] * scale, both[1] * scale
        hid_all[my_tile] = (gate / (1.0 + jnp.exp(-gate)) * up).astype(BF16)
        for offset in ALL:
            copy_to(hid_all.at[my_tile], hid_all.at[my_tile], 7, peer(*offset))
        waiter(hid_all.at[pl.ds(0, tiles_ff - 1)], 7).wait_recv()

    @pl.when(my_tile >= tiles_ff)
    def _():
        waiter(hid_all, 7).wait_recv()

    copies[14].wait()
    active = jnp.concatenate([hid_all[t] for t in range(tiles_ff)], axis=1)
    term = jnp.dot(active, wdown[...], preferred_element_type=F32)
    out_ref[...] = (stream + over_heads(term, last_send, last_recv, 8)).astype(BF16)

    waiter(qkv_recv.at[pl.ds(0, len(ALL))], 0).wait_send()
    waiter(q_all.at[pl.ds(0, len(NEAR))], 1).wait_send()
    waiter(part_recv.at[pl.ds(0, len(ALL))], 2).wait_send()
    waiter(attn_all.at[pl.ds(0, len(NEAR))], 3).wait_send()
    waiter(head_recv.at[pl.ds(0, len(HEADS))], 4).wait_send()
    waiter(last_recv.at[pl.ds(0, len(HEADS))], 8).wait_send()

    @pl.when(my_tile < tiles_ff)
    def _():
        waiter(ff_recv.at[pl.ds(0, tiles_ff - 1)], 5).wait_send()
        waiter(square_recv.at[pl.ds(0, tiles_ff - 1)], 6).wait_send()
        waiter(part_recv.at[pl.ds(0, N - 1)], 7).wait_send()

    @pl.when(my_tile >= tiles_ff)
    def _():
        waiter(ff_recv.at[pl.ds(0, tiles_ff)], 5).wait_send()
        waiter(square_recv.at[pl.ds(0, tiles_ff)], 6).wait_send()


def on_device(
    hidden_in,
    attn_gain,
    query_key_value_weight,
    k_cache,
    value_cache,
    page_table,
    lengths,
    output_weight,
    mlp_gain,
    w_in,
    w_down,
):
    width = hidden_in.shape[1]
    ff = w_down.shape[0]
    tiles_ff = -(-ff // LANES)
    half = D // 2
    inverse = ROPE_BASE ** (-np.arange(half, dtype=np.float64) * (2.0 / D))
    inverse = np.broadcast_to(np.concatenate([inverse, inverse]), (8, D)).astype(np.float32)
    slots = k_cache.shape[1]
    return pl.pallas_call(
        functools.partial(kernel, tiles_ff, ff),
        out_shape=jax.ShapeDtypeStruct((B, width), BF16),
        in_specs=[pl.BlockSpec(memory_space=pl.ANY)] * 12,
        out_specs=pl.BlockSpec(memory_space=pltpu.VMEM),
        scratch_shapes=[
            pltpu.VMEM((B, width), BF16),
            pltpu.VMEM((width,), BF16),
            pltpu.VMEM((width,), BF16),
            pltpu.VMEM((8, D), F32),
            pltpu.SMEM((PAGES_HERE, B), jnp.int32),
            pltpu.SMEM((B,), jnp.int32),
            pltpu.VMEM((width, VECTORS * D), BF16),
            pltpu.VMEM((slots, PAGE, D), BF16),
            pltpu.VMEM((slots, PAGE, D), BF16),
            pltpu.VMEM((G * D, width), BF16),
            pltpu.VMEM((2, tiles_ff * LANES, width), BF16),
            pltpu.VMEM((tiles_ff * LANES, width), BF16),
            pltpu.VMEM((B * 2 * G, D), F32),
            pltpu.VMEM((B, 2 * G, D), BF16),
            pltpu.VMEM((N, 2 * G, D), BF16),
            pltpu.VMEM((B, G, D), BF16),
            pltpu.VMEM((B, 2 * G, D), BF16),
            pltpu.VMEM((N, 2 * G, D), BF16),
            pltpu.VMEM((B, G, D), BF16),
            pltpu.VMEM((B * G, D), F32),
            pltpu.VMEM((B, width), BF16),
            pltpu.VMEM((H, B, width), BF16),
            pltpu.VMEM((N, 2, B, LANES), BF16),
            pltpu.VMEM((N, 2, B, LANES), BF16),
            pltpu.VMEM((1, LANES), F32),
            pltpu.VMEM((N, 1, LANES), F32),
            pltpu.VMEM((tiles_ff, B, LANES), BF16),
            pltpu.VMEM((B, width), BF16),
            pltpu.VMEM((H, B, width), BF16),
            pltpu.SemaphoreType.DMA((15,)),
            pltpu.SemaphoreType.DMA((9,)),
            pltpu.SemaphoreType.DMA((9,)),
        ],
        compiler_params=pltpu.CompilerParams(collective_id=0, has_side_effects=True),
    )(
        hidden_in,
        attn_gain,
        query_key_value_weight.transpose(1, 0, 2)[0],
        k_cache[0],
        value_cache[0],
        page_table.T,
        lengths,
        output_weight[0],
        mlp_gain,
        w_in.transpose(1, 2, 0),
        w_down,
        jnp.asarray(inverse),
    )


def solution(mesh):
    return jax.shard_map(
        on_device,
        mesh=mesh,
        in_specs=(
            P(None, "kvp"),
            P("kvp"),
            P("kvp", "head", None),
            P("head", "kvp", None, None),
            P("head", "kvp", None, None),
            P(None, "kvp"),
            P(),
            P("head", None, "kvp"),
            P("kvp"),
            P("kvp", None, "head"),
            P("head", "kvp"),
        ),
        out_specs=P(None, "kvp"),
        check_vma=False,
    )
```

```python
import functools
import math

import jax
import jax.numpy as jnp
import numpy as np
from jax import lax
from jax.experimental import pallas as pl
from jax.experimental.pallas import tpu as pltpu
from jax.sharding import PartitionSpec as P

MESH = pl.DeviceIdType.MESH
F32 = jnp.float32
BF16 = jnp.bfloat16

MODEL_WIDTH = 8192
EPSILON = 1e-05
ROPE_BASE = 10000.0
B = 16
G = 8
D = 128
Z, X = 8, 4
N = Z * X
Y, C = 4, 2
H = Y * C
PAGE = 128
PAGES_HERE = 4
VECTORS = G + 2
LANES = 128
SQUARE_ROW = VECTORS
GROUP = 7
OWNERS = 16
SPREAD, UNSPREAD = 5, 13


def around(offset, size):
    return min(offset % size, -offset % size)


def far_first(offsets, sizes):
    return sorted(offsets, key=lambda at: -sum(around(o, s) for o, s in zip(at, sizes)))


ALL = far_first([(dz, dx) for dz in range(Z) for dx in range(X) if (dz, dx) != (0, 0)], (Z, X))
NEAR = far_first(
    [(dz, dx) for dz in (-1, 0, 1, 2) for dx in range(X) if (dz, dx) != (0, 0)], (Z, X)
)
HEADS = far_first([(dy, dc) for dy in range(Y) for dc in range(C) if (dy, dc) != (0, 0)], (Y, C))


def iota(shape, dim):
    return lax.broadcasted_iota(jnp.int32, shape, dim)


def to_row(column):
    wide = jnp.broadcast_to(column, (B, LANES))
    kept = jnp.where(iota((B, LANES), 0) == iota((B, LANES), 1), wide, 0.0)
    return jnp.sum(kept, axis=0, keepdims=True)


def to_column(row):
    wide = jnp.broadcast_to(row, (B, LANES))
    kept = jnp.where(iota((B, LANES), 0) == iota((B, LANES), 1), wide, 0.0)
    return jnp.sum(kept, axis=1, keepdims=True)


def rounded(value):
    return value.astype(BF16).astype(F32)


def sine_and_cosine(angle):
    turns = jnp.floor(angle * (1.0 / (2.0 * math.pi)) + 0.5)
    left = angle - turns * 6.28125
    left = left - turns * (2.0 * math.pi - 6.28125)
    y = left * 0.5
    z = y * y
    sine, cosine = 0.0, 0.0
    for k in range(6, -1, -1):
        sine = sine * z + (-1.0) ** k / math.factorial(2 * k + 1)
    sine = sine * y
    for k in range(7, -1, -1):
        cosine = cosine * z + (-1.0) ** k / math.factorial(2 * k)
    return 2.0 * sine * cosine, 1.0 - 2.0 * sine * sine


def kernel(
    tiles_ff,
    ff,
    hidden_hbm,
    attn_gain_hbm,
    qkv_hbm,
    k_hbm,
    v_hbm,
    table_hbm,
    lengths_hbm,
    wo_hbm,
    mlp_gain_hbm,
    win_hbm,
    wdown_hbm,
    inverse_hbm,
    out_ref,
    hidden,
    attn_gain,
    mlp_gain,
    inverse,
    table,
    lengths,
    wqkv,
    keys,
    values,
    wo,
    win,
    wdown,
    turned,
    qkv_send,
    qkv_recv,
    q_all,
    pair,
    part_send,
    part_recv,
    attn_all,
    attn_rows,
    head_send,
    head_recv,
    ff_send,
    ff_recv,
    square_send,
    square_recv,
    hid_all,
    last_send,
    last_recv,
    local_sem,
    send_sem,
    recv_sem,
):
    me = lax.axis_index("kvp")
    my_head = lax.axis_index("head")
    my_z, my_x = me // X, lax.rem(me, X)
    my_y, my_c = my_head // C, lax.rem(my_head, C)
    zs = [lax.rem(my_z + dz, Z) for dz in range(Z)]
    xs = [lax.rem(my_x + dx, X) for dx in range(X)]
    ys = [lax.rem(my_y + dy, Y) for dy in range(Y)]
    cs = [lax.rem(my_c + dc, C) for dc in range(C)]

    def peer(dz, dx):
        return {"kvp": zs[dz % Z] * X + xs[dx % X]}

    def head_peer(dy, dc):
        return {"head": ys[dy] * C + cs[dc]}

    request_of_z = [lax.rem(z, Z // 2) * X for z in zs]

    def request_at(dz, dx):
        return request_of_z[dz % Z] + xs[dx % X]

    my_request = request_at(0, 0)
    my_tile = lax.rem(me * UNSPREAD, N)

    def copy_to(src, dst, phase, device):
        pltpu.make_async_remote_copy(
            src_ref=src,
            dst_ref=dst,
            send_sem=send_sem.at[phase],
            recv_sem=recv_sem.at[phase],
            device_id=device,
            device_id_type=MESH,
        ).start()

    def waiter(ref, phase):
        return pltpu.make_async_remote_copy(
            src_ref=ref,
            dst_ref=ref,
            send_sem=send_sem.at[phase],
            recv_sem=recv_sem.at[phase],
            device_id=peer(1, 0),
            device_id_type=MESH,
        )

    pairs = [
        (hidden_hbm, hidden),
        (attn_gain_hbm, attn_gain),
        (qkv_hbm, wqkv),
        (lengths_hbm, lengths),
        (inverse_hbm, inverse),
        (table_hbm, table),
        (k_hbm.at[pl.ds(0, 32)], keys.at[pl.ds(0, 32)]),
        (k_hbm.at[pl.ds(32, 32)], keys.at[pl.ds(32, 32)]),
        (v_hbm.at[pl.ds(0, 32)], values.at[pl.ds(0, 32)]),
        (v_hbm.at[pl.ds(32, 32)], values.at[pl.ds(32, 32)]),
        (wo_hbm, wo),
        (mlp_gain_hbm, mlp_gain),
        (win_hbm.at[0], win.at[0, pl.ds(0, ff)]),
        (win_hbm.at[1], win.at[1, pl.ds(0, ff)]),
        (wdown_hbm, wdown.at[pl.ds(0, ff)]),
    ]
    copies = [
        pltpu.make_async_copy(src, dst, local_sem.at[at]) for at, (src, dst) in enumerate(pairs)
    ]
    for copy in copies[:3]:
        copy.start()
    barrier = pltpu.get_barrier_semaphore()

    @pl.when(me < OWNERS)
    def _():
        for offset in ALL:
            pl.semaphore_signal(barrier, inc=1, device_id=peer(*offset), device_id_type=MESH)

    for offset in HEADS:
        pl.semaphore_signal(barrier, inc=1, device_id=head_peer(*offset), device_id_type=MESH)
    for copy in copies[3:]:
        copy.start()

    pad = win.shape[1] - ff
    win[:, pl.ds(ff, pad), :] = jnp.zeros((2, pad, win.shape[2]), BF16)
    wdown[pl.ds(ff, pad), :] = jnp.zeros((pad, wdown.shape[1]), BF16)
    turned[...] = jnp.zeros(turned.shape, F32)

    for copy in copies[:3]:
        copy.wait()
    x = hidden[...].astype(F32)
    normed = (x * attn_gain[...][None, :].astype(F32)).astype(BF16)
    partial = jnp.dot(normed, wqkv[...], preferred_element_type=F32)
    for v in range(VECTORS):
        turned[pl.ds(v, B, stride=2 * G), :] = partial[:, v * D : (v + 1) * D]
    square = jnp.sum(x * x, axis=1, keepdims=True)
    high = rounded(square)
    turned[pl.ds(SQUARE_ROW, B, stride=2 * G), :] = jnp.where(
        iota((B, LANES), 1) < LANES // 2, high, square - high
    )
    qkv_send[...] = turned[...].reshape(B, 2 * G, D).astype(BF16)
    pl.semaphore_wait(barrier, jnp.where(me < OWNERS, OWNERS - 1, OWNERS) + len(HEADS))

    def send_qkv(step):
        owner = lax.rem(me + step, OWNERS)
        copy_to(qkv_send.at[owner], qkv_recv.at[me], 0, {"kvp": owner})

    for step in range(1, OWNERS):
        send_qkv(step)

    @pl.when(me >= OWNERS)
    def _():
        send_qkv(0)

    for copy in copies[3:6]:
        copy.wait()
    sine, cosine = sine_and_cosine(lengths[my_request].astype(F32) * inverse[...])
    lane = iota((G, LANES), 1)
    sine = jnp.where(lane < D // 2, -sine, sine)[0:1]
    cosine = cosine[0:1]
    for copy in copies[6:10]:
        copy.wait()

    @pl.when(me < OWNERS)
    def _():
        qkv_recv[me] = qkv_send[my_request]
        waiter(qkv_recv.at[pl.ds(0, N - 1)], 0).wait_recv()
        total = jnp.sum(qkv_recv[...].astype(F32), axis=0)
        square = total[SQUARE_ROW : SQUARE_ROW + 1]
        square = square[:, 0:1] + square[:, LANES // 2 : LANES // 2 + 1]
        total = total * lax.rsqrt(square / MODEL_WIDTH + EPSILON)
        rotated = total * cosine + pltpu.roll(total, D // 2, 1) * sine
        q_all[my_request] = rotated[:G].astype(BF16)
        for offset in ALL:
            copy_to(q_all.at[my_request], q_all.at[my_request], 1, peer(*offset))
        pair[...] = jnp.where(iota((G, LANES), 0) == 0, rotated[G:], total[G:]).astype(BF16)
        copy_to(pair, pair, 9, peer(Z // 2, 0))
        waiter(q_all.at[pl.ds(0, OWNERS - 1)], 1).wait_recv()

    @pl.when(me >= OWNERS)
    def _():
        waiter(q_all, 1).wait_recv()

    factor = D ** (-0.5)
    first = me * (PAGES_HERE * PAGE)
    slots = [[table[p, b] for p in range(PAGES_HERE)] for b in range(B)]
    scores = [
        [
            lax.dot_general(
                q_all[b], keys[slot], (((1,), (1,)), ((), ())), preferred_element_type=F32
            )
            for slot in slots[b]
        ]
        for b in range(B)
    ]
    parts = []
    for b in range(B):
        left = lengths[b] - first
        live = [lane + p * PAGE < left for p in range(PAGES_HERE)]
        masked = [jnp.where(ok, s * factor, -1e30) for ok, s in zip(live, scores[b])]
        top = jnp.max(functools.reduce(jnp.maximum, masked), axis=1, keepdims=True)
        weights = [jnp.where(ok, jnp.exp(s - top), 0.0) for ok, s in zip(live, masked)]
        total = jnp.sum(functools.reduce(jnp.add, weights), axis=1, keepdims=True)
        summed = 0.0
        for p in range(PAGES_HERE):
            summed = summed + jnp.dot(
                weights[p].astype(BF16), values[slots[b][p]], preferred_element_type=F32
            )
        high = rounded(top)
        middle = rounded(top - high)
        low = top - high - middle
        stats = jnp.where(
            lane < 32, high, jnp.where(lane < 64, middle, jnp.where(lane < 96, low, total))
        )
        parts.append(jnp.concatenate([summed, stats], axis=0).astype(BF16))
    for b in range(B):
        part_send[b] = parts[b]

    for offset in ALL:
        copy_to(part_send.at[request_at(*offset)], part_recv.at[me], 2, peer(*offset))
    part_recv[me] = part_send[my_request]
    copies[10].wait()

    @pl.when(me >= OWNERS)
    def _():
        waiter(pair, 9).wait_recv()

    new_key, new_value = pair[...].astype(F32)[0:1], pair[...].astype(F32)[1:2]
    own = jnp.sum(q_all[my_request].astype(F32) * new_key, axis=1, keepdims=True) * factor
    waiter(part_recv.at[pl.ds(0, len(ALL))], 2).wait_recv()
    tops, overall = [], own
    for k in range(N):
        stats = part_recv[k].astype(F32)[G:]
        tops.append(stats[:, 0:1] + stats[:, 32:33] + stats[:, 64:65])
        overall = jnp.maximum(overall, tops[k])
    own_weight = jnp.exp(own - overall)
    total = own_weight
    summed = rounded(own_weight) * new_value
    for k in range(N):
        tile = part_recv[k].astype(F32)
        carried = jnp.exp(tops[k] - overall)
        total = total + tile[G:, 96:97] * carried
        summed = summed + tile[:G] * carried
    attn_all[my_request] = (summed / total).astype(BF16)
    for offset in NEAR:
        copy_to(attn_all.at[my_request], attn_all.at[my_request], 3, peer(*offset))
    waiter(attn_all.at[pl.ds(0, len(NEAR))], 3).wait_recv()

    attn_rows[...] = attn_all[...].astype(F32).reshape(B * G, D)
    attn = jnp.concatenate(
        [attn_rows[pl.ds(g, B, stride=G), :].astype(BF16) for g in range(G)], axis=1
    )

    def over_heads(term, send_ref, recv_ref, phase):
        send_ref[...] = term.astype(BF16)
        for offset in HEADS:
            copy_to(send_ref, recv_ref.at[my_head], phase, head_peer(*offset))
        recv_ref[my_head] = term.astype(BF16)
        waiter(recv_ref.at[pl.ds(0, len(HEADS))], phase).wait_recv()
        return jnp.sum(recv_ref[...].astype(F32), axis=0)

    term = jnp.dot(attn, wo[...], preferred_element_type=F32)
    for copy in copies[11:14]:
        copy.wait()
    stream = x + over_heads(term, head_send, head_recv, 4)

    square_row = to_row(jnp.sum(stream * stream, axis=1, keepdims=True))
    square_send[...] = square_row
    normed = (stream * mlp_gain[...][None, :].astype(F32)).astype(BF16)
    tiles = [lax.rem(my_tile + step, tiles_ff) for step in range(tiles_ff)]
    owners = [{"kvp": lax.rem(tile * SPREAD, N)} for tile in tiles]

    def send_square(step):
        copy_to(square_send, square_recv.at[me], 6, owners[step])

    def make(step):
        rows = pl.ds(pl.multiple_of(tiles[step] * LANES, LANES), LANES)
        for part in range(2):
            ff_send[tiles[step], part] = lax.dot_general(
                normed,
                win[part, rows, :],
                (((1,), (1,)), ((), ())),
                preferred_element_type=F32,
            ).astype(BF16)

    def send(step):
        copy_to(ff_send.at[tiles[step]], ff_recv.at[me], 5, owners[step])

    for step in range(1, tiles_ff):
        send_square(step)
    for start in range(1, tiles_ff, GROUP):
        for step in range(start, min(start + GROUP, tiles_ff)):
            make(step)
        for step in range(start, min(start + GROUP, tiles_ff)):
            send(step)
    make(0)

    @pl.when(my_tile >= tiles_ff)
    def _():
        send_square(0)
        send(0)

    @pl.when(my_tile < tiles_ff)
    def _():
        ff_recv[me] = ff_send[my_tile]
        square_recv[me] = square_row
        waiter(square_recv.at[pl.ds(0, N - 1)], 6).wait_recv()
        waiter(ff_recv.at[pl.ds(0, N - 1)], 5).wait_recv()
        square = to_column(jnp.sum(square_recv[...], axis=0))
        scale = lax.rsqrt(square / MODEL_WIDTH + EPSILON)
        both = jnp.sum(ff_recv[...].astype(F32), axis=0)
        gate, up = both[0] * scale, both[1] * scale
        hid_all[my_tile] = (gate / (1.0 + jnp.exp(-gate)) * up).astype(BF16)
        for offset in ALL:
            copy_to(hid_all.at[my_tile], hid_all.at[my_tile], 7, peer(*offset))
        waiter(hid_all.at[pl.ds(0, tiles_ff - 1)], 7).wait_recv()

    @pl.when(my_tile >= tiles_ff)
    def _():
        waiter(hid_all, 7).wait_recv()

    copies[14].wait()
    active = jnp.concatenate([hid_all[t] for t in range(tiles_ff)], axis=1)
    term = jnp.dot(active, wdown[...], preferred_element_type=F32)
    out_ref[...] = (stream + over_heads(term, last_send, last_recv, 8)).astype(BF16)

    @pl.when(me < OWNERS)
    def _():
        waiter(qkv_recv.at[pl.ds(0, OWNERS - 1)], 0).wait_send()
        waiter(qkv_recv.at[pl.ds(0, N - 1), pl.ds(0, G)], 1).wait_send()
        waiter(pair, 9).wait_send()

    @pl.when(me >= OWNERS)
    def _():
        waiter(qkv_recv.at[pl.ds(0, OWNERS)], 0).wait_send()

    waiter(part_recv.at[pl.ds(0, len(ALL))], 2).wait_send()
    waiter(attn_all.at[pl.ds(0, len(NEAR))], 3).wait_send()
    waiter(head_recv.at[pl.ds(0, len(HEADS))], 4).wait_send()
    waiter(last_recv.at[pl.ds(0, len(HEADS))], 8).wait_send()

    @pl.when(my_tile < tiles_ff)
    def _():
        waiter(ff_recv.at[pl.ds(0, tiles_ff - 1)], 5).wait_send()
        waiter(square_recv.at[pl.ds(0, tiles_ff - 1)], 6).wait_send()
        waiter(part_recv.at[pl.ds(0, N - 1)], 7).wait_send()

    @pl.when(my_tile >= tiles_ff)
    def _():
        waiter(ff_recv.at[pl.ds(0, tiles_ff)], 5).wait_send()
        waiter(square_recv.at[pl.ds(0, tiles_ff)], 6).wait_send()


def on_device(
    hidden_in,
    attn_gain,
    query_key_value_weight,
    k_cache,
    value_cache,
    page_table,
    lengths,
    output_weight,
    mlp_gain,
    w_in,
    w_down,
):
    width = hidden_in.shape[1]
    ff = w_down.shape[0]
    tiles_ff = -(-ff // LANES)
    half = D // 2
    inverse = ROPE_BASE ** (-np.arange(half, dtype=np.float64) * (2.0 / D))
    inverse = np.broadcast_to(np.concatenate([inverse, inverse]), (8, D)).astype(np.float32)
    slots = k_cache.shape[1]
    return pl.pallas_call(
        functools.partial(kernel, tiles_ff, ff),
        out_shape=pltpu.VMEM((B, width), BF16),
        in_specs=[pl.BlockSpec(memory_space=pl.ANY)] * 12,
        out_specs=pl.BlockSpec(memory_space=pltpu.VMEM),
        scratch_shapes=[
            pltpu.VMEM((B, width), BF16),
            pltpu.VMEM((width,), BF16),
            pltpu.VMEM((width,), BF16),
            pltpu.VMEM((8, D), F32),
            pltpu.SMEM((PAGES_HERE, B), jnp.int32),
            pltpu.SMEM((B,), jnp.int32),
            pltpu.VMEM((width, VECTORS * D), BF16),
            pltpu.VMEM((slots, PAGE, D), BF16),
            pltpu.VMEM((slots, PAGE, D), BF16),
            pltpu.VMEM((G * D, width), BF16),
            pltpu.VMEM((2, tiles_ff * LANES, width), BF16),
            pltpu.VMEM((tiles_ff * LANES, width), BF16),
            pltpu.VMEM((B * 2 * G, D), F32),
            pltpu.VMEM((B, 2 * G, D), BF16),
            pltpu.VMEM((N, 2 * G, D), BF16),
            pltpu.VMEM((B, G, D), BF16),
            pltpu.VMEM((G, D), BF16),
            pltpu.VMEM((B, 2 * G, D), BF16),
            pltpu.VMEM((N, 2 * G, D), BF16),
            pltpu.VMEM((B, G, D), BF16),
            pltpu.VMEM((B * G, D), F32),
            pltpu.VMEM((B, width), BF16),
            pltpu.VMEM((H, B, width), BF16),
            pltpu.VMEM((tiles_ff, 2, B, LANES), BF16),
            pltpu.VMEM((N, 2, B, LANES), BF16),
            pltpu.VMEM((1, LANES), F32),
            pltpu.VMEM((N, 1, LANES), F32),
            pltpu.VMEM((tiles_ff, B, LANES), BF16),
            pltpu.VMEM((B, width), BF16),
            pltpu.VMEM((H, B, width), BF16),
            pltpu.SemaphoreType.DMA((15,)),
            pltpu.SemaphoreType.DMA((10,)),
            pltpu.SemaphoreType.DMA((10,)),
        ],
        compiler_params=pltpu.CompilerParams(collective_id=0, has_side_effects=True),
    )(
        hidden_in,
        attn_gain,
        query_key_value_weight.transpose(1, 0, 2)[0],
        k_cache[0],
        value_cache[0],
        page_table.T,
        lengths,
        output_weight[0],
        mlp_gain,
        w_in.transpose(1, 2, 0),
        w_down,
        jnp.asarray(inverse),
    )


def solution(mesh):
    return jax.shard_map(
        on_device,
        mesh=mesh,
        in_specs=(
            P(None, "kvp"),
            P("kvp"),
            P("kvp", "head", None),
            P("head", "kvp", None, None),
            P("head", "kvp", None, None),
            P(None, "kvp"),
            P(),
            P("head", None, "kvp"),
            P("kvp"),
            P("kvp", None, "head"),
            P("head", "kvp"),
        ),
        out_specs=P(None, "kvp"),
        check_vma=False,
    )
```

```python
import functools
import math

import jax
import jax.numpy as jnp
import numpy as np
from jax import lax
from jax.experimental import pallas as pl
from jax.experimental.pallas import tpu as pltpu
from jax.sharding import PartitionSpec as P

MESH = pl.DeviceIdType.MESH
F32 = jnp.float32
BF16 = jnp.bfloat16

MODEL_WIDTH = 8192
EPSILON = 1e-05
ROPE_BASE = 10000.0
B = 16
G = 8
D = 128
Z, X = 8, 4
N = Z * X
Y, C = 4, 2
H = Y * C
PAGE = 128
PAGES_HERE = 4
VECTORS = G + 2
LANES = 128
SQUARE_ROW = VECTORS
GROUPS = (4, 6, 6, 5)
OWNERS = 16
SPREAD, UNSPREAD = 5, 13


def around(offset, size):
    return min(offset % size, -offset % size)


def far_first(offsets, sizes):
    return sorted(offsets, key=lambda at: -sum(around(o, s) for o, s in zip(at, sizes)))


ALL = far_first([(dz, dx) for dz in range(Z) for dx in range(X) if (dz, dx) != (0, 0)], (Z, X))
NEAR = far_first(
    [(dz, dx) for dz in (-1, 0, 1, 2) for dx in range(X) if (dz, dx) != (0, 0)], (Z, X)
)
HEADS = far_first([(dy, dc) for dy in range(Y) for dc in range(C) if (dy, dc) != (0, 0)], (Y, C))


def iota(shape, dim):
    return lax.broadcasted_iota(jnp.int32, shape, dim)


def to_row(column):
    wide = jnp.broadcast_to(column, (B, LANES))
    kept = jnp.where(iota((B, LANES), 0) == iota((B, LANES), 1), wide, 0.0)
    return jnp.sum(kept, axis=0, keepdims=True)


def to_column(row):
    wide = jnp.broadcast_to(row, (B, LANES))
    kept = jnp.where(iota((B, LANES), 0) == iota((B, LANES), 1), wide, 0.0)
    return jnp.sum(kept, axis=1, keepdims=True)


def rounded(value):
    return value.astype(BF16).astype(F32)


def sine_and_cosine(angle):
    turns = jnp.floor(angle * (1.0 / (2.0 * math.pi)) + 0.5)
    left = angle - turns * 6.28125
    left = left - turns * (2.0 * math.pi - 6.28125)
    y = left * 0.5
    z = y * y
    sine, cosine = 0.0, 0.0
    for k in range(6, -1, -1):
        sine = sine * z + (-1.0) ** k / math.factorial(2 * k + 1)
    sine = sine * y
    for k in range(7, -1, -1):
        cosine = cosine * z + (-1.0) ** k / math.factorial(2 * k)
    return 2.0 * sine * cosine, 1.0 - 2.0 * sine * sine


def kernel(
    tiles_ff,
    ff,
    hidden_hbm,
    attn_gain_hbm,
    qkv_hbm,
    k_hbm,
    v_hbm,
    table_hbm,
    lengths_hbm,
    wo_hbm,
    mlp_gain_hbm,
    win_hbm,
    wdown_hbm,
    inverse_hbm,
    out_ref,
    hidden,
    attn_gain,
    mlp_gain,
    inverse,
    table,
    lengths,
    wqkv,
    keys,
    values,
    wo,
    win,
    wdown,
    turned,
    qkv_send,
    qkv_recv,
    q_all,
    pair,
    part_send,
    part_recv,
    attn_all,
    attn_rows,
    head_send,
    head_recv,
    ff_send,
    ff_recv,
    square_send,
    square_recv,
    hid_all,
    last_send,
    last_recv,
    owners,
    tiles,
    local_sem,
    send_sem,
    recv_sem,
):
    me = lax.axis_index("kvp")
    my_head = lax.axis_index("head")
    my_z, my_x = me // X, lax.rem(me, X)
    my_y, my_c = my_head // C, lax.rem(my_head, C)
    zs = [lax.rem(my_z + dz, Z) for dz in range(Z)]
    xs = [lax.rem(my_x + dx, X) for dx in range(X)]
    ys = [lax.rem(my_y + dy, Y) for dy in range(Y)]
    cs = [lax.rem(my_c + dc, C) for dc in range(C)]

    def peer(dz, dx):
        return {"kvp": zs[dz % Z] * X + xs[dx % X]}

    def head_peer(dy, dc):
        return {"head": ys[dy] * C + cs[dc]}

    request_of_z = [lax.rem(z, Z // 2) * X for z in zs]

    def request_at(dz, dx):
        return request_of_z[dz % Z] + xs[dx % X]

    my_request = request_at(0, 0)
    my_tile = lax.rem(me * UNSPREAD, N)

    def copy_to(src, dst, phase, device):
        pltpu.make_async_remote_copy(
            src_ref=src,
            dst_ref=dst,
            send_sem=send_sem.at[phase],
            recv_sem=recv_sem.at[phase],
            device_id=device,
            device_id_type=MESH,
        ).start()

    def waiter(ref, phase):
        return pltpu.make_async_remote_copy(
            src_ref=ref,
            dst_ref=ref,
            send_sem=send_sem.at[phase],
            recv_sem=recv_sem.at[phase],
            device_id=peer(1, 0),
            device_id_type=MESH,
        )

    pairs = [
        (hidden_hbm, hidden),
        (attn_gain_hbm, attn_gain),
        (qkv_hbm, wqkv),
        (lengths_hbm, lengths),
        (inverse_hbm, inverse),
        (table_hbm, table),
        (k_hbm.at[pl.ds(0, 32)], keys.at[pl.ds(0, 32)]),
        (k_hbm.at[pl.ds(32, 32)], keys.at[pl.ds(32, 32)]),
        (v_hbm.at[pl.ds(0, 32)], values.at[pl.ds(0, 32)]),
        (v_hbm.at[pl.ds(32, 32)], values.at[pl.ds(32, 32)]),
        (wo_hbm, wo),
        (mlp_gain_hbm, mlp_gain),
        (win_hbm.at[0], win.at[0, pl.ds(0, ff)]),
        (win_hbm.at[1], win.at[1, pl.ds(0, ff)]),
        (wdown_hbm, wdown.at[pl.ds(0, ff)]),
    ]
    copies = [
        pltpu.make_async_copy(src, dst, local_sem.at[at]) for at, (src, dst) in enumerate(pairs)
    ]
    for copy in copies[:3]:
        copy.start()
    barrier = pltpu.get_barrier_semaphore()

    @pl.when(me < OWNERS)
    def _():
        for offset in ALL:
            pl.semaphore_signal(barrier, inc=1, device_id=peer(*offset), device_id_type=MESH)

    for offset in HEADS:
        pl.semaphore_signal(barrier, inc=1, device_id=head_peer(*offset), device_id_type=MESH)
    for copy in copies[3:]:
        copy.start()

    count, count_ff = 0, 0
    for offset in ALL:
        device = peer(*offset)["kvp"]
        owners[count] = device
        count = count + jnp.where(device < OWNERS, 1, 0)
        tile = lax.rem(device * UNSPREAD, N)
        tiles[count_ff] = tile
        count_ff = count_ff + jnp.where(tile < tiles_ff, 1, 0)

    @pl.when(my_tile < tiles_ff)
    def _():
        tiles[tiles_ff - 1] = my_tile

    pad = win.shape[1] - ff
    win[:, pl.ds(ff, pad), :] = jnp.zeros((2, pad, win.shape[2]), BF16)
    wdown[pl.ds(ff, pad), :] = jnp.zeros((pad, wdown.shape[1]), BF16)
    turned[...] = jnp.zeros(turned.shape, F32)

    for copy in copies[:3]:
        copy.wait()
    x = hidden[...].astype(F32)
    normed = (x * attn_gain[...][None, :].astype(F32)).astype(BF16)
    partial = jnp.dot(normed, wqkv[...], preferred_element_type=F32)
    for v in range(VECTORS):
        turned[pl.ds(v, B, stride=2 * G), :] = partial[:, v * D : (v + 1) * D]
    square = jnp.sum(x * x, axis=1, keepdims=True)
    high = rounded(square)
    turned[pl.ds(SQUARE_ROW, B, stride=2 * G), :] = jnp.where(
        iota((B, LANES), 1) < LANES // 2, high, square - high
    )
    qkv_send[...] = turned[...].reshape(B, 2 * G, D).astype(BF16)
    pl.semaphore_wait(barrier, jnp.where(me < OWNERS, OWNERS - 1, OWNERS) + len(HEADS))

    def send_qkv(step):
        owner = owners[step]
        copy_to(qkv_send.at[owner], qkv_recv.at[me], 0, {"kvp": owner})

    for step in range(OWNERS - 1):
        send_qkv(step)

    @pl.when(me >= OWNERS)
    def _():
        send_qkv(OWNERS - 1)

    for copy in copies[3:6]:
        copy.wait()
    sine, cosine = sine_and_cosine(lengths[my_request].astype(F32) * inverse[...])
    lane = iota((G, LANES), 1)
    sine = jnp.where(lane < D // 2, -sine, sine)[0:1]
    cosine = cosine[0:1]
    for copy in copies[6:10]:
        copy.wait()

    @pl.when(me < OWNERS)
    def _():
        qkv_recv[me] = qkv_send[my_request]
        waiter(qkv_recv.at[pl.ds(0, N - 1)], 0).wait_recv()
        total = jnp.sum(qkv_recv[...].astype(F32), axis=0)
        square = total[SQUARE_ROW : SQUARE_ROW + 1]
        square = square[:, 0:1] + square[:, LANES // 2 : LANES // 2 + 1]
        total = total * lax.rsqrt(square / MODEL_WIDTH + EPSILON)
        rotated = total * cosine + pltpu.roll(total, D // 2, 1) * sine
        q_all[my_request] = rotated[:G].astype(BF16)
        for offset in ALL:
            copy_to(q_all.at[my_request], q_all.at[my_request], 1, peer(*offset))
        pair[...] = jnp.where(iota((G, LANES), 0) == 0, rotated[G:], total[G:]).astype(BF16)
        copy_to(pair, pair, 9, peer(Z // 2, 0))
        waiter(q_all.at[pl.ds(0, OWNERS - 1)], 1).wait_recv()

    @pl.when(me >= OWNERS)
    def _():
        waiter(q_all, 1).wait_recv()

    factor = D ** (-0.5)
    first = me * (PAGES_HERE * PAGE)
    slots = [[table[p, b] for p in range(PAGES_HERE)] for b in range(B)]
    scores = [
        [
            lax.dot_general(
                q_all[b], keys[slot], (((1,), (1,)), ((), ())), preferred_element_type=F32
            )
            for slot in slots[b]
        ]
        for b in range(B)
    ]
    parts = []
    for b in range(B):
        left = lengths[b] - first
        live = [lane + p * PAGE < left for p in range(PAGES_HERE)]
        masked = [jnp.where(ok, s * factor, -1e30) for ok, s in zip(live, scores[b])]
        top = jnp.max(functools.reduce(jnp.maximum, masked), axis=1, keepdims=True)
        weights = [jnp.where(ok, jnp.exp(s - top), 0.0) for ok, s in zip(live, masked)]
        total = jnp.sum(functools.reduce(jnp.add, weights), axis=1, keepdims=True)
        summed = 0.0
        for p in range(PAGES_HERE):
            summed = summed + jnp.dot(
                weights[p].astype(BF16), values[slots[b][p]], preferred_element_type=F32
            )
        high = rounded(top)
        middle = rounded(top - high)
        low = top - high - middle
        stats = jnp.where(
            lane < 32, high, jnp.where(lane < 64, middle, jnp.where(lane < 96, low, total))
        )
        parts.append(jnp.concatenate([summed, stats], axis=0).astype(BF16))
    for b in range(B):
        part_send[b] = parts[b]

    for offset in ALL:
        copy_to(part_send.at[request_at(*offset)], part_recv.at[me], 2, peer(*offset))
    part_recv[me] = part_send[my_request]
    copies[10].wait()

    @pl.when(me >= OWNERS)
    def _():
        waiter(pair, 9).wait_recv()

    new_key, new_value = pair[...].astype(F32)[0:1], pair[...].astype(F32)[1:2]
    own = jnp.sum(q_all[my_request].astype(F32) * new_key, axis=1, keepdims=True) * factor
    waiter(part_recv.at[pl.ds(0, len(ALL))], 2).wait_recv()
    tops, overall = [], own
    for k in range(N):
        stats = part_recv[k].astype(F32)[G:]
        tops.append(stats[:, 0:1] + stats[:, 32:33] + stats[:, 64:65])
        overall = jnp.maximum(overall, tops[k])
    own_weight = jnp.exp(own - overall)
    total = own_weight
    summed = rounded(own_weight) * new_value
    for k in range(N):
        tile = part_recv[k].astype(F32)
        carried = jnp.exp(tops[k] - overall)
        total = total + tile[G:, 96:97] * carried
        summed = summed + tile[:G] * carried
    attn_all[my_request] = (summed / total).astype(BF16)
    for offset in NEAR:
        copy_to(attn_all.at[my_request], attn_all.at[my_request], 3, peer(*offset))
    waiter(attn_all.at[pl.ds(0, len(NEAR))], 3).wait_recv()

    attn_rows[...] = attn_all[...].astype(F32).reshape(B * G, D)
    attn = jnp.concatenate(
        [attn_rows[pl.ds(g, B, stride=G), :].astype(BF16) for g in range(G)], axis=1
    )

    def over_heads(term, send_ref, recv_ref, phase):
        send_ref[...] = term.astype(BF16)
        for offset in HEADS:
            copy_to(send_ref, recv_ref.at[my_head], phase, head_peer(*offset))
        recv_ref[my_head] = term.astype(BF16)
        waiter(recv_ref.at[pl.ds(0, len(HEADS))], phase).wait_recv()
        return jnp.sum(recv_ref[...].astype(F32), axis=0)

    term = jnp.dot(attn, wo[...], preferred_element_type=F32)
    for copy in copies[11:14]:
        copy.wait()
    stream = x + over_heads(term, head_send, head_recv, 4)

    square_row = to_row(jnp.sum(stream * stream, axis=1, keepdims=True))
    square_send[...] = square_row
    normed = (stream * mlp_gain[...][None, :].astype(F32)).astype(BF16)
    ours = [tiles[step] for step in range(tiles_ff)]

    def owner_of(step):
        return {"kvp": lax.rem(ours[step] * SPREAD, N)}

    def send_square(step):
        copy_to(square_send, square_recv.at[me], 6, owner_of(step))

    def make(step):
        rows = pl.ds(pl.multiple_of(ours[step] * LANES, LANES), LANES)
        for part in range(2):
            ff_send[ours[step], part] = lax.dot_general(
                normed,
                win[part, rows, :],
                (((1,), (1,)), ((), ())),
                preferred_element_type=F32,
            ).astype(BF16)

    def send(step):
        copy_to(ff_send.at[ours[step]], ff_recv.at[me], 5, owner_of(step))

    start = 0
    for size in GROUPS:
        for step in range(start, start + size):
            make(step)
        for step in range(start, start + size):
            send(step)
            send_square(step)
        start += size
    make(start)

    @pl.when(my_tile >= tiles_ff)
    def _():
        send(start)
        send_square(start)

    @pl.when(my_tile < tiles_ff)
    def _():
        ff_recv[me] = ff_send[my_tile]
        square_recv[me] = square_row
        waiter(square_recv.at[pl.ds(0, N - 1)], 6).wait_recv()
        waiter(ff_recv.at[pl.ds(0, N - 1)], 5).wait_recv()
        square = to_column(jnp.sum(square_recv[...], axis=0))
        scale = lax.rsqrt(square / MODEL_WIDTH + EPSILON)
        both = jnp.sum(ff_recv[...].astype(F32), axis=0)
        gate, up = both[0] * scale, both[1] * scale
        hid_all[my_tile] = (gate / (1.0 + jnp.exp(-gate)) * up).astype(BF16)
        for offset in ALL:
            copy_to(hid_all.at[my_tile], hid_all.at[my_tile], 7, peer(*offset))
        waiter(hid_all.at[pl.ds(0, tiles_ff - 1)], 7).wait_recv()

    @pl.when(my_tile >= tiles_ff)
    def _():
        waiter(hid_all, 7).wait_recv()

    copies[14].wait()
    active = jnp.concatenate([hid_all[t] for t in range(tiles_ff)], axis=1)
    term = jnp.dot(active, wdown[...], preferred_element_type=F32)
    out_ref[...] = (stream + over_heads(term, last_send, last_recv, 8)).astype(BF16)

    @pl.when(me < OWNERS)
    def _():
        waiter(qkv_recv.at[pl.ds(0, OWNERS - 1)], 0).wait_send()
        waiter(qkv_recv.at[pl.ds(0, N - 1), pl.ds(0, G)], 1).wait_send()
        waiter(pair, 9).wait_send()

    @pl.when(me >= OWNERS)
    def _():
        waiter(qkv_recv.at[pl.ds(0, OWNERS)], 0).wait_send()

    waiter(part_recv.at[pl.ds(0, len(ALL))], 2).wait_send()
    waiter(attn_all.at[pl.ds(0, len(NEAR))], 3).wait_send()
    waiter(head_recv.at[pl.ds(0, len(HEADS))], 4).wait_send()
    waiter(last_recv.at[pl.ds(0, len(HEADS))], 8).wait_send()

    @pl.when(my_tile < tiles_ff)
    def _():
        waiter(ff_recv.at[pl.ds(0, tiles_ff - 1)], 5).wait_send()
        waiter(square_recv.at[pl.ds(0, tiles_ff - 1)], 6).wait_send()
        waiter(part_recv.at[pl.ds(0, N - 1)], 7).wait_send()

    @pl.when(my_tile >= tiles_ff)
    def _():
        waiter(ff_recv.at[pl.ds(0, tiles_ff)], 5).wait_send()
        waiter(square_recv.at[pl.ds(0, tiles_ff)], 6).wait_send()


def on_device(
    hidden_in,
    attn_gain,
    query_key_value_weight,
    k_cache,
    value_cache,
    page_table,
    lengths,
    output_weight,
    mlp_gain,
    w_in,
    w_down,
):
    width = hidden_in.shape[1]
    ff = w_down.shape[0]
    tiles_ff = -(-ff // LANES)
    half = D // 2
    inverse = ROPE_BASE ** (-np.arange(half, dtype=np.float64) * (2.0 / D))
    inverse = np.broadcast_to(np.concatenate([inverse, inverse]), (8, D)).astype(np.float32)
    slots = k_cache.shape[1]
    return pl.pallas_call(
        functools.partial(kernel, tiles_ff, ff),
        out_shape=pltpu.VMEM((B, width), BF16),
        in_specs=[pl.BlockSpec(memory_space=pl.ANY)] * 12,
        out_specs=pl.BlockSpec(memory_space=pltpu.VMEM),
        scratch_shapes=[
            pltpu.VMEM((B, width), BF16),
            pltpu.VMEM((width,), BF16),
            pltpu.VMEM((width,), BF16),
            pltpu.VMEM((8, D), F32),
            pltpu.SMEM((PAGES_HERE, B), jnp.int32),
            pltpu.SMEM((B,), jnp.int32),
            pltpu.VMEM((width, VECTORS * D), BF16),
            pltpu.VMEM((slots, PAGE, D), BF16),
            pltpu.VMEM((slots, PAGE, D), BF16),
            pltpu.VMEM((G * D, width), BF16),
            pltpu.VMEM((2, tiles_ff * LANES, width), BF16),
            pltpu.VMEM((tiles_ff * LANES, width), BF16),
            pltpu.VMEM((B * 2 * G, D), F32),
            pltpu.VMEM((B, 2 * G, D), BF16),
            pltpu.VMEM((N, 2 * G, D), BF16),
            pltpu.VMEM((B, G, D), BF16),
            pltpu.VMEM((G, D), BF16),
            pltpu.VMEM((B, 2 * G, D), BF16),
            pltpu.VMEM((N, 2 * G, D), BF16),
            pltpu.VMEM((B, G, D), BF16),
            pltpu.VMEM((B * G, D), F32),
            pltpu.VMEM((B, width), BF16),
            pltpu.VMEM((H, B, width), BF16),
            pltpu.VMEM((tiles_ff, 2, B, LANES), BF16),
            pltpu.VMEM((N, 2, B, LANES), BF16),
            pltpu.VMEM((1, LANES), F32),
            pltpu.VMEM((N, 1, LANES), F32),
            pltpu.VMEM((tiles_ff, B, LANES), BF16),
            pltpu.VMEM((B, width), BF16),
            pltpu.VMEM((H, B, width), BF16),
            pltpu.SMEM((N,), jnp.int32),
            pltpu.SMEM((N,), jnp.int32),
            pltpu.SemaphoreType.DMA((15,)),
            pltpu.SemaphoreType.DMA((10,)),
            pltpu.SemaphoreType.DMA((10,)),
        ],
        compiler_params=pltpu.CompilerParams(collective_id=0, has_side_effects=True),
    )(
        hidden_in,
        attn_gain,
        query_key_value_weight.transpose(1, 0, 2)[0],
        k_cache[0],
        value_cache[0],
        page_table.T,
        lengths,
        output_weight[0],
        mlp_gain,
        w_in.transpose(1, 2, 0),
        w_down,
        jnp.asarray(inverse),
    )


def solution(mesh):
    return jax.shard_map(
        on_device,
        mesh=mesh,
        in_specs=(
            P(None, "kvp"),
            P("kvp"),
            P("kvp", "head", None),
            P("head", "kvp", None, None),
            P("head", "kvp", None, None),
            P(None, "kvp"),
            P(),
            P("head", None, "kvp"),
            P("kvp"),
            P("kvp", None, "head"),
            P("head", "kvp"),
        ),
        out_specs=P(None, "kvp"),
        check_vma=False,
    )
```

```python
import functools
import math

import jax
import jax.numpy as jnp
import numpy as np
from jax import lax
from jax.experimental import pallas as pl
from jax.experimental.pallas import tpu as pltpu
from jax.sharding import PartitionSpec as P

MESH = pl.DeviceIdType.MESH
F32 = jnp.float32
BF16 = jnp.bfloat16

MODEL_WIDTH = 8192
EPSILON = 1e-05
ROPE_BASE = 10000.0
B = 16
G = 8
D = 128
Z, X = 8, 4
N = Z * X
Y, C = 4, 2
H = Y * C
PAGE = 128
PAGES_HERE = 4
VECTORS = G + 2
LANES = 128
TURNS = 8
TILE = 120
SQUARE_ROW = VECTORS
GROUPS = (4, 6, 6, 6)
OWNERS = 16
SUMMING = 1
SPREAD, UNSPREAD = 5, 13


def around(offset, size):
    return min(offset % size, -offset % size)


def far_first(offsets, sizes):
    return sorted(offsets, key=lambda at: -sum(around(o, s) for o, s in zip(at, sizes)))


ALL = far_first([(dz, dx) for dz in range(Z) for dx in range(X) if (dz, dx) != (0, 0)], (Z, X))
NEAR = far_first(
    [(dz, dx) for dz in (-1, 0, 1, 2) for dx in range(X) if (dz, dx) != (0, 0)], (Z, X)
)
HEADS = far_first([(dy, dc) for dy in range(Y) for dc in range(C) if (dy, dc) != (0, 0)], (Y, C))


ROWS = OWNERS // X
NEAREST_ROWS = [sorted(range(ROWS), key=lambda row: around(row - z, Z)) for z in range(Z)]


def iota(shape, dim):
    return lax.broadcasted_iota(jnp.int32, shape, dim)


def rounded(value):
    return value.astype(BF16).astype(F32)


def sine_and_cosine(angle):
    turns = jnp.floor(angle * (1.0 / (2.0 * math.pi)) + 0.5)
    left = angle - turns * 6.28125
    left = left - turns * (2.0 * math.pi - 6.28125)
    y = left * 0.5
    z = y * y
    sine, cosine = 0.0, 0.0
    for k in range(6, -1, -1):
        sine = sine * z + (-1.0) ** k / math.factorial(2 * k + 1)
    sine = sine * y
    for k in range(7, -1, -1):
        cosine = cosine * z + (-1.0) ** k / math.factorial(2 * k)
    return 2.0 * sine * cosine, 1.0 - 2.0 * sine * sine


def kernel(
    tiles_ff,
    ff,
    hidden_hbm,
    attn_gain_hbm,
    qkv_hbm,
    k_hbm,
    v_hbm,
    table_hbm,
    lengths_hbm,
    wo_hbm,
    mlp_gain_hbm,
    win_hbm,
    wdown_hbm,
    inverse_hbm,
    out_ref,
    hidden,
    attn_gain,
    mlp_gain,
    inverse,
    table,
    lengths,
    wqkv,
    keys,
    values,
    keys_across,
    wo,
    win,
    win_across,
    wdown,
    turned,
    qkv_send,
    qkv_recv,
    q_all,
    tile,
    part_send,
    part_recv,
    joined,
    attn_all,
    attn_rows,
    head_send,
    head_recv,
    ff_send,
    ff_recv,
    units,
    hid_all,
    last_send,
    last_recv,
    owners,
    tiles,
    local_sem,
    query_sem,
    sum_sem,
    tile_sem,
    all_sem,
    send_sem,
    recv_sem,
):
    me = lax.axis_index("kvp")
    my_head = lax.axis_index("head")
    my_z, my_x = me // X, lax.rem(me, X)
    my_y, my_c = my_head // C, lax.rem(my_head, C)
    zs = [lax.rem(my_z + dz, Z) for dz in range(Z)]
    xs = [lax.rem(my_x + dx, X) for dx in range(X)]
    ys = [lax.rem(my_y + dy, Y) for dy in range(Y)]
    cs = [lax.rem(my_c + dc, C) for dc in range(C)]

    sums = my_c == SUMMING

    def at(kvp, plane):
        return {"kvp": kvp, "head": my_y * C + plane}

    def kvp_at(dz, dx):
        return zs[dz % Z] * X + xs[dx % X]

    def head_peer(dy, dc):
        return {"head": ys[dy] * C + cs[dc]}

    request_of_z = [lax.rem(z, Z // 2) * X for z in zs]

    def request_at(dz, dx):
        return request_of_z[dz % Z] + xs[dx % X]

    my_request = request_at(0, 0)
    my_tile = lax.rem(me * UNSPREAD, N)

    def copy_to(src, dst, phase, device, arrival=None):
        pltpu.make_async_remote_copy(
            src_ref=src,
            dst_ref=dst,
            send_sem=send_sem.at[phase],
            recv_sem=recv_sem.at[phase] if arrival is None else arrival,
            device_id=device,
            device_id_type=MESH,
        ).start()

    def waiter(ref, phase, arrival=None):
        return pltpu.make_async_remote_copy(
            src_ref=ref,
            dst_ref=ref,
            send_sem=send_sem.at[phase],
            recv_sem=recv_sem.at[phase] if arrival is None else arrival,
            device_id={"kvp": kvp_at(1, 0)},
            device_id_type=MESH,
        )

    pairs = [
        (hidden_hbm, hidden),
        (attn_gain_hbm, attn_gain),
        (qkv_hbm, wqkv),
        (lengths_hbm, lengths),
        (inverse_hbm, inverse),
        (table_hbm, table),
        (k_hbm.at[pl.ds(0, 32)], keys.at[pl.ds(0, 32)]),
        (k_hbm.at[pl.ds(32, 32)], keys.at[pl.ds(32, 32)]),
        (v_hbm.at[pl.ds(0, 32)], values.at[pl.ds(0, 32)]),
        (v_hbm.at[pl.ds(32, 32)], values.at[pl.ds(32, 32)]),
        (wo_hbm, wo),
        (mlp_gain_hbm, mlp_gain),
        (win_hbm.at[0], win.at[0, pl.ds(0, ff)]),
        (win_hbm.at[1], win.at[1, pl.ds(0, ff)]),
        (wdown_hbm, wdown.at[pl.ds(0, ff)]),
    ]
    copies = [
        pltpu.make_async_copy(src, dst, local_sem.at[at]) for at, (src, dst) in enumerate(pairs)
    ]
    for copy in copies[:3]:
        copy.start()
    barrier = pltpu.get_barrier_semaphore()

    @pl.when(sums & (me < OWNERS))
    def _():
        for offset in ALL:
            for plane in range(C):
                pl.semaphore_signal(
                    barrier, inc=1, device_id=at(kvp_at(*offset), plane), device_id_type=MESH
                )
        pl.semaphore_signal(barrier, inc=1, device_id=at(me, 0), device_id_type=MESH)

    for offset in HEADS:
        pl.semaphore_signal(barrier, inc=1, device_id=head_peer(*offset), device_id_type=MESH)
    for copy in copies[3:]:
        copy.start()

    count, count_ff = 0, 0
    for offset in ALL:
        device = kvp_at(*offset)
        owners[count] = device
        count = count + jnp.where(device < OWNERS, 1, 0)
        candidate = lax.rem(device * UNSPREAD, N)
        tiles[count_ff] = candidate
        count_ff = count_ff + jnp.where(candidate < tiles_ff, 1, 0)

    @pl.when(me < OWNERS)
    def _():
        owners[OWNERS - 1] = me

    @pl.when(my_tile < tiles_ff)
    def _():
        tiles[tiles_ff - 1] = my_tile

    pad = win.shape[1] - ff
    win[:, pl.ds(ff, pad), :] = jnp.zeros((2, pad, win.shape[2]), BF16)
    wdown[pl.ds(ff, pad), :] = jnp.zeros((pad, wdown.shape[1]), BF16)
    turned[...] = jnp.zeros(turned.shape, F32)

    for copy in copies[:3]:
        copy.wait()
    x = hidden[...].astype(F32)
    normed = (x * attn_gain[...][None, :].astype(F32)).astype(BF16)
    partial = jnp.dot(normed, wqkv[...], preferred_element_type=F32)
    for v in range(VECTORS):
        turned[pl.ds(v, B, stride=2 * G), :] = partial[:, v * D : (v + 1) * D]
    square = jnp.sum(x * x, axis=1, keepdims=True)
    high = rounded(square)
    turned[pl.ds(SQUARE_ROW, B, stride=2 * G), :] = jnp.where(
        iota((B, LANES), 1) < LANES // 2, high, square - high
    )
    qkv_send[...] = turned[...].reshape(B, 2 * G, D).astype(BF16)
    pl.semaphore_wait(
        barrier, jnp.where(sums & (me < OWNERS), OWNERS - 1, OWNERS) + len(HEADS)
    )

    def send_qkv(step):
        owner = owners[step]
        copy_to(
            qkv_send.at[owner],
            qkv_recv.at[my_c, me],
            0,
            at(owner, SUMMING),
            sum_sem.at[0, my_c],
        )

    for step in range(OWNERS - 1):
        send_qkv(step)

    @pl.when((me >= OWNERS) | (my_c != SUMMING))
    def _():
        send_qkv(OWNERS - 1)

    for copy in copies[3:6]:
        copy.wait()
    sine, cosine = sine_and_cosine(lengths[my_request].astype(F32) * inverse[...])
    lane = iota((G, LANES), 1)
    sine = jnp.where(lane < D // 2, -sine, sine)[0:1]
    cosine = cosine[0:1]
    for copy in copies[6:10]:
        copy.wait()

    @pl.loop(0, keys.shape[0] // TURNS)
    def _(step):
        for turn in range(TURNS):
            keys_across[step * TURNS + turn] = keys[step * TURNS + turn].T

    for copy in copies[11:14]:
        copy.wait()
    for t in range(tiles_ff):
        for part in range(2):
            win_across[t, part] = win[part, pl.ds(t * TILE, LANES), :].T


    def wait_parts(recv_ref, phase, plane):
        arrived = recv_ref.at[plane] if plane != SUMMING else recv_ref.at[plane, pl.ds(0, N - 1)]
        waiter(arrived, 0, sum_sem.at[phase, plane]).wait_recv()

    @pl.when(sums & (me < OWNERS))
    def _():
        qkv_recv[SUMMING, me] = qkv_send[my_request]
        for plane in (SUMMING, 1 - SUMMING):
            wait_parts(qkv_recv, 0, plane)
            total = jnp.sum(qkv_recv[plane].astype(F32), axis=0)
            square = total[SQUARE_ROW : SQUARE_ROW + 1]
            square = square[:, 0:1] + square[:, LANES // 2 : LANES // 2 + 1]
            total = total * lax.rsqrt(square / MODEL_WIDTH + EPSILON)
            rotated = total * cosine + pltpu.roll(total, D // 2, 1) * sine
            tile[plane] = jnp.where(iota((2 * G, LANES), 0) <= G, rotated, total).astype(BF16)
            for offset in ALL + [(0, 0)]:
                if offset != (0, 0) or plane != SUMMING:
                    copy_to(
                        tile.at[plane, pl.ds(0, G)],
                        q_all.at[me],
                        1 + plane,
                        at(kvp_at(*offset), plane),
                        query_sem.at[my_z],
                    )
            copy_to(
                tile.at[plane],
                tile.at[plane],
                3 + plane,
                at(kvp_at(Z // 2, 0), SUMMING),
                tile_sem.at[plane],
            )
        q_all[me] = tile[SUMMING, pl.ds(0, G)]

    factor = D ** (-0.5)
    first = me * (PAGES_HERE * PAGE)

    def attend(requests):
        slots = [[table[p, b] for p in range(PAGES_HERE)] for b in requests]
        queries = [q_all[b] for b in requests]
        scores = [
            [
                jnp.dot(query, keys_across[slot], preferred_element_type=F32)
                for slot in here
            ]
            for query, here in zip(queries, slots)
        ]
        parts = []
        for b, here, products in zip(requests, slots, scores):
            left = lengths[b] - first
            live = [lane + p * PAGE < left for p in range(PAGES_HERE)]
            masked = [jnp.where(ok, s * factor, -1e30) for ok, s in zip(live, products)]
            top = jnp.max(functools.reduce(jnp.maximum, masked), axis=1, keepdims=True)
            weights = [jnp.where(ok, jnp.exp(s - top), 0.0) for ok, s in zip(live, masked)]
            total = jnp.sum(functools.reduce(jnp.add, weights), axis=1, keepdims=True)
            summed = 0.0
            for p in range(PAGES_HERE):
                summed = summed + jnp.dot(
                    weights[p].astype(BF16), values[here[p]], preferred_element_type=F32
                )
            high = rounded(top)
            middle = rounded(top - high)
            low = top - high - middle
            stats = jnp.where(
                lane < 32, high, jnp.where(lane < 64, middle, jnp.where(lane < 96, low, total))
            )
            parts.append(jnp.concatenate([summed, stats], axis=0).astype(BF16))
        for b, part in zip(requests, parts):
            part_send[b] = part

    def send_part(request, target):
        copy_to(
            part_send.at[request],
            part_recv.at[my_c, me],
            5,
            at(target, SUMMING),
            sum_sem.at[1, my_c],
        )

    for place in range(ROWS):
        row = 0
        for z in range(Z):
            row = jnp.where(my_z == z, NEAREST_ROWS[z][place], row)
        requests = [row * X + x for x in range(X)]
        if place == 0:

            @pl.when(sums & (me < OWNERS))
            def _(row=row):
                waiter(q_all.at[pl.ds(0, X - 1)], 0, query_sem.at[row]).wait_recv()

            @pl.when(jnp.logical_not(sums & (me < OWNERS)))
            def _(row=row):
                waiter(q_all.at[pl.ds(0, X)], 0, query_sem.at[row]).wait_recv()

        else:
            waiter(q_all.at[pl.ds(0, X)], 0, query_sem.at[row]).wait_recv()
        attend(requests)
        for request in requests:
            for target in (request + OWNERS, request):

                @pl.when((me != target) | (my_c != SUMMING))
                def _(request=request, target=target):
                    send_part(request, target)

    copies[10].wait()

    @pl.when(sums)
    def _():
        part_recv[SUMMING, me] = part_send[my_request]
        for plane in (SUMMING, 1 - SUMMING):

            @pl.when(me >= OWNERS)
            def _(plane=plane):
                waiter(tile.at[plane], 0, tile_sem.at[plane]).wait_recv()

            known = tile[plane].astype(F32)
            new_key, new_value = known[G : G + 1], known[G + 1 : G + 2]
            own = jnp.sum(known[:G] * new_key, axis=1, keepdims=True) * factor
            wait_parts(part_recv, 1, plane)
            tops, overall = [], own
            for k in range(N):
                stats = part_recv[plane, k].astype(F32)[G:]
                tops.append(stats[:, 0:1] + stats[:, 32:33] + stats[:, 64:65])
                overall = jnp.maximum(overall, tops[k])
            own_weight = jnp.exp(own - overall)
            total = own_weight
            summed = rounded(own_weight) * new_value
            for k in range(N):
                part = part_recv[plane, k].astype(F32)
                carried = jnp.exp(tops[k] - overall)
                total = total + part[G:, 96:97] * carried
                summed = summed + part[:G] * carried
            joined[plane] = (summed / total).astype(BF16)
            for offset in NEAR + [(0, 0)]:
                if offset != (0, 0) or plane != SUMMING:
                    copy_to(
                        joined.at[plane],
                        attn_all.at[my_request],
                        6 + plane,
                        at(kvp_at(*offset), plane),
                        all_sem.at[0],
                    )
        attn_all[my_request] = joined[SUMMING]
        waiter(attn_all.at[pl.ds(0, len(NEAR))], 0, all_sem.at[0]).wait_recv()

    @pl.when(my_c != SUMMING)
    def _():
        waiter(attn_all, 0, all_sem.at[0]).wait_recv()

    attn_rows[...] = attn_all[...].astype(F32).reshape(B * G, D)
    attn = jnp.concatenate(
        [attn_rows[pl.ds(g, B, stride=G), :].astype(BF16) for g in range(G)], axis=1
    )

    def over_heads(term, send_ref, recv_ref, phase):
        send_ref[...] = term.astype(BF16)
        for offset in HEADS:
            copy_to(send_ref, recv_ref.at[my_head], phase, head_peer(*offset))
        recv_ref[my_head] = term.astype(BF16)
        waiter(recv_ref.at[pl.ds(0, len(HEADS))], phase).wait_recv()
        return jnp.sum(recv_ref[...].astype(F32), axis=0)

    term = jnp.dot(attn, wo[...], preferred_element_type=F32)
    stream = x + over_heads(term, head_send, head_recv, 8)

    square = jnp.sum(stream * stream, axis=1, keepdims=True)
    high = rounded(square)
    column = iota((B, LANES), 1)
    normed = (stream * mlp_gain[...][None, :].astype(F32)).astype(BF16)
    ours = [tiles[step] for step in range(tiles_ff)]

    def make(step):
        for part in range(2):
            product = jnp.dot(normed, win_across[ours[step], part], preferred_element_type=F32)
            rest = jnp.where(column == TILE, high, square - high) if part == 0 else 0.0
            ff_send[ours[step], part] = jnp.where(column < TILE, product, rest).astype(BF16)

    def send(step):
        copy_to(
            ff_send.at[ours[step]],
            ff_recv.at[my_c, me],
            10,
            at(lax.rem(ours[step] * SPREAD, N), SUMMING),
            sum_sem.at[2, my_c],
        )

    start = 0
    for size in GROUPS:
        for step in range(start, start + size):
            make(step)
        for step in range(start, start + size):
            send(step)
        start += size
    make(start)

    @pl.when((my_tile >= tiles_ff) | (my_c != SUMMING))
    def _():
        send(start)

    summing_tile = sums & (my_tile < tiles_ff)

    @pl.when(summing_tile)
    def _():
        ff_recv[SUMMING, me] = ff_send[my_tile]
        for plane in (SUMMING, 1 - SUMMING):
            wait_parts(ff_recv, 2, plane)
            both = jnp.sum(ff_recv[plane].astype(F32), axis=0)
            square = both[0][:, TILE : TILE + 1] + both[0][:, TILE + 1 : TILE + 2]
            scale = lax.rsqrt(square / MODEL_WIDTH + EPSILON)
            gate, up = both[0] * scale, both[1] * scale
            active = gate / (1.0 + jnp.exp(-gate)) * up
            units[plane] = jnp.where(column < TILE, active, 0.0).astype(BF16)
            for offset in ALL + [(0, 0)]:
                if offset != (0, 0) or plane != SUMMING:
                    copy_to(
                        units.at[plane],
                        hid_all.at[my_tile],
                        11 + plane,
                        at(kvp_at(*offset), plane),
                        all_sem.at[1],
                    )
        hid_all[my_tile] = units[SUMMING]
        waiter(hid_all.at[pl.ds(0, tiles_ff - 1)], 0, all_sem.at[1]).wait_recv()

    @pl.when(jnp.logical_not(summing_tile))
    def _():
        waiter(hid_all, 0, all_sem.at[1]).wait_recv()

    copies[14].wait()
    term = 0.0
    for t in range(tiles_ff):
        term = term + jnp.dot(
            hid_all[t], wdown[pl.ds(t * TILE, LANES), :], preferred_element_type=F32
        )
    out_ref[...] = (stream + over_heads(term, last_send, last_recv, 9)).astype(BF16)

    @pl.when(sums & (me < OWNERS))
    def _():
        waiter(qkv_recv.at[0, pl.ds(0, OWNERS - 1)], 0).wait_send()
        for plane in range(C):
            count = N if plane != SUMMING else N - 1
            waiter(qkv_recv.at[0, pl.ds(0, count), pl.ds(0, G)], 1 + plane).wait_send()
            waiter(tile.at[plane], 3 + plane).wait_send()

    @pl.when(jnp.logical_not(sums & (me < OWNERS)))
    def _():
        waiter(qkv_recv.at[0, pl.ds(0, OWNERS)], 0).wait_send()

    @pl.when(sums)
    def _():
        waiter(part_recv.at[0, pl.ds(0, N - 1)], 5).wait_send()
        for plane in range(C):
            count = len(NEAR) + (plane != SUMMING)
            waiter(attn_all.at[pl.ds(0, count)], 6 + plane).wait_send()

    @pl.when(my_c != SUMMING)
    def _():
        waiter(part_recv.at[0], 5).wait_send()

    waiter(head_recv.at[pl.ds(0, len(HEADS))], 8).wait_send()
    waiter(last_recv.at[pl.ds(0, len(HEADS))], 9).wait_send()

    @pl.when(summing_tile)
    def _():
        waiter(ff_recv.at[0, pl.ds(0, tiles_ff - 1)], 10).wait_send()
        for plane in range(C):
            count = N if plane != SUMMING else N - 1
            waiter(part_recv.at[0, pl.ds(0, count)], 11 + plane).wait_send()

    @pl.when(jnp.logical_not(summing_tile))
    def _():
        waiter(ff_recv.at[0, pl.ds(0, tiles_ff)], 10).wait_send()


def on_device(
    hidden_in,
    attn_gain,
    query_key_value_weight,
    k_cache,
    value_cache,
    page_table,
    lengths,
    output_weight,
    mlp_gain,
    w_in,
    w_down,
):
    width = hidden_in.shape[1]
    ff = w_down.shape[0]
    tiles_ff = -(-ff // TILE)
    half = D // 2
    inverse = ROPE_BASE ** (-np.arange(half, dtype=np.float64) * (2.0 / D))
    inverse = np.broadcast_to(np.concatenate([inverse, inverse]), (8, D)).astype(np.float32)
    slots = k_cache.shape[1]
    return pl.pallas_call(
        functools.partial(kernel, tiles_ff, ff),
        out_shape=pltpu.VMEM((B, width), BF16),
        in_specs=[pl.BlockSpec(memory_space=pl.ANY)] * 12,
        out_specs=pl.BlockSpec(memory_space=pltpu.VMEM),
        scratch_shapes=[
            pltpu.VMEM((B, width), BF16),
            pltpu.VMEM((width,), BF16),
            pltpu.VMEM((width,), BF16),
            pltpu.VMEM((8, D), F32),
            pltpu.SMEM((PAGES_HERE, B), jnp.int32),
            pltpu.SMEM((B,), jnp.int32),
            pltpu.VMEM((width, VECTORS * D), BF16),
            pltpu.VMEM((slots, PAGE, D), BF16),
            pltpu.VMEM((slots, PAGE, D), BF16),
            pltpu.VMEM((slots, D, PAGE), BF16),
            pltpu.VMEM((G * D, width), BF16),
            pltpu.VMEM((2, (tiles_ff - 1) * TILE + LANES, width), BF16),
            pltpu.VMEM((tiles_ff, 2, width, LANES), BF16),
            pltpu.VMEM(((tiles_ff - 1) * TILE + LANES, width), BF16),
            pltpu.VMEM((B * 2 * G, D), F32),
            pltpu.VMEM((B, 2 * G, D), BF16),
            pltpu.VMEM((C, N, 2 * G, D), BF16),
            pltpu.VMEM((B, G, D), BF16),
            pltpu.VMEM((C, 2 * G, D), BF16),
            pltpu.VMEM((B, 2 * G, D), BF16),
            pltpu.VMEM((C, N, 2 * G, D), BF16),
            pltpu.VMEM((C, G, D), BF16),
            pltpu.VMEM((B, G, D), BF16),
            pltpu.VMEM((B * G, D), F32),
            pltpu.VMEM((B, width), BF16),
            pltpu.VMEM((H, B, width), BF16),
            pltpu.VMEM((tiles_ff, 2, B, LANES), BF16),
            pltpu.VMEM((C, N, 2, B, LANES), BF16),
            pltpu.VMEM((C, B, LANES), BF16),
            pltpu.VMEM((tiles_ff, B, LANES), BF16),
            pltpu.VMEM((B, width), BF16),
            pltpu.VMEM((H, B, width), BF16),
            pltpu.SMEM((N,), jnp.int32),
            pltpu.SMEM((N,), jnp.int32),
            pltpu.SemaphoreType.DMA((15,)),
            pltpu.SemaphoreType.DMA((ROWS,)),
            pltpu.SemaphoreType.DMA((3, C)),
            pltpu.SemaphoreType.DMA((C,)),
            pltpu.SemaphoreType.DMA((2,)),
            pltpu.SemaphoreType.DMA((13,)),
            pltpu.SemaphoreType.DMA((13,)),
        ],
        compiler_params=pltpu.CompilerParams(collective_id=0, has_side_effects=True),
    )(
        hidden_in,
        attn_gain,
        query_key_value_weight.transpose(1, 0, 2)[0],
        k_cache[0],
        value_cache[0],
        page_table.T,
        lengths,
        output_weight[0],
        mlp_gain,
        w_in.transpose(1, 2, 0),
        w_down,
        jnp.asarray(inverse),
    )


def solution(mesh):
    return jax.shard_map(
        on_device,
        mesh=mesh,
        in_specs=(
            P(None, "kvp"),
            P("kvp"),
            P("kvp", "head", None),
            P("head", "kvp", None, None),
            P("head", "kvp", None, None),
            P(None, "kvp"),
            P(),
            P("head", None, "kvp"),
            P("kvp"),
            P("kvp", None, "head"),
            P("head", "kvp"),
        ),
        out_specs=P(None, "kvp"),
        check_vma=False,
    )
```

```python
import functools
import math

import jax
import jax.numpy as jnp
import numpy as np
from jax import lax
from jax.experimental import pallas as pl
from jax.experimental.pallas import tpu as pltpu
from jax.sharding import PartitionSpec as P

MESH = pl.DeviceIdType.MESH
F32 = jnp.float32
BF16 = jnp.bfloat16

MODEL_WIDTH = 8192
EPSILON = 1e-05
ROPE_BASE = 10000.0
B = 16
G = 8
D = 128
Z, X = 8, 4
N = Z * X
Y, C = 4, 2
H = Y * C
PAGE = 128
PAGES_HERE = 4
VECTORS = G + 2
LANES = 128
TURNS = 8
TILE = 120
SQUARE_ROW = VECTORS
REST = 4
GROUPS = (4, 6, 6, 6)
OWNERS = 16
SUMMING = 1
SPREAD, UNSPREAD = 5, 13


def around(offset, size):
    return min(offset % size, -offset % size)


def far_first(offsets, sizes):
    return sorted(offsets, key=lambda at: -sum(around(o, s) for o, s in zip(at, sizes)))


ALL = far_first([(dz, dx) for dz in range(Z) for dx in range(X) if (dz, dx) != (0, 0)], (Z, X))
NEAR = far_first(
    [(dz, dx) for dz in (-1, 0, 1, 2) for dx in range(X) if (dz, dx) != (0, 0)], (Z, X)
)
HEADS = far_first([(dy, dc) for dy in range(Y) for dc in range(C) if (dy, dc) != (0, 0)], (Y, C))


ROWS = OWNERS // X
NEAREST_ROWS = [sorted(range(ROWS), key=lambda row: around(row - z, Z)) for z in range(Z)]


def iota(shape, dim):
    return lax.broadcasted_iota(jnp.int32, shape, dim)


def rounded(value):
    return value.astype(BF16).astype(F32)


def sine_and_cosine(angle):
    turns = jnp.floor(angle * (1.0 / (2.0 * math.pi)) + 0.5)
    left = angle - turns * 6.28125
    left = left - turns * (2.0 * math.pi - 6.28125)
    y = left * 0.5
    z = y * y
    sine, cosine = 0.0, 0.0
    for k in range(6, -1, -1):
        sine = sine * z + (-1.0) ** k / math.factorial(2 * k + 1)
    sine = sine * y
    for k in range(7, -1, -1):
        cosine = cosine * z + (-1.0) ** k / math.factorial(2 * k)
    return 2.0 * sine * cosine, 1.0 - 2.0 * sine * sine


def kernel(
    tiles_ff,
    ff,
    hidden_hbm,
    attn_gain_hbm,
    qkv_hbm,
    k_hbm,
    v_hbm,
    table_hbm,
    lengths_hbm,
    wo_hbm,
    mlp_gain_hbm,
    win_hbm,
    wdown_hbm,
    inverse_hbm,
    out_ref,
    hidden,
    attn_gain,
    mlp_gain,
    inverse,
    table,
    lengths,
    wqkv,
    keys,
    values,
    keys_across,
    wo,
    win,
    win_across,
    wdown,
    turned,
    qkv_send,
    qkv_recv,
    rest_send,
    rest_recv,
    q_all,
    tile,
    part_send,
    part_recv,
    joined,
    attn_all,
    attn_rows,
    head_send,
    head_recv,
    ff_send,
    ff_recv,
    units,
    hid_all,
    last_send,
    last_recv,
    owners,
    tiles,
    local_sem,
    query_sem,
    sum_sem,
    tile_sem,
    all_sem,
    send_sem,
    recv_sem,
):
    me = lax.axis_index("kvp")
    my_head = lax.axis_index("head")
    my_z, my_x = me // X, lax.rem(me, X)
    my_y, my_c = my_head // C, lax.rem(my_head, C)
    zs = [lax.rem(my_z + dz, Z) for dz in range(Z)]
    xs = [lax.rem(my_x + dx, X) for dx in range(X)]
    ys = [lax.rem(my_y + dy, Y) for dy in range(Y)]
    cs = [lax.rem(my_c + dc, C) for dc in range(C)]

    sums = my_c == SUMMING

    def at(kvp, plane):
        return {"kvp": kvp, "head": my_y * C + plane}

    def kvp_at(dz, dx):
        return zs[dz % Z] * X + xs[dx % X]

    def head_peer(dy, dc):
        return {"head": ys[dy] * C + cs[dc]}

    request_of_z = [lax.rem(z, Z // 2) * X for z in zs]

    def request_at(dz, dx):
        return request_of_z[dz % Z] + xs[dx % X]

    my_request = request_at(0, 0)
    my_tile = lax.rem(me * UNSPREAD, N)

    def copy_to(src, dst, phase, device, arrival=None):
        pltpu.make_async_remote_copy(
            src_ref=src,
            dst_ref=dst,
            send_sem=send_sem.at[phase],
            recv_sem=recv_sem.at[phase] if arrival is None else arrival,
            device_id=device,
            device_id_type=MESH,
        ).start()

    def waiter(ref, phase, arrival=None):
        return pltpu.make_async_remote_copy(
            src_ref=ref,
            dst_ref=ref,
            send_sem=send_sem.at[phase],
            recv_sem=recv_sem.at[phase] if arrival is None else arrival,
            device_id={"kvp": kvp_at(1, 0)},
            device_id_type=MESH,
        )

    pairs = [
        (hidden_hbm, hidden),
        (attn_gain_hbm, attn_gain),
        (qkv_hbm, wqkv),
        (lengths_hbm, lengths),
        (inverse_hbm, inverse),
        (table_hbm, table),
        (k_hbm.at[pl.ds(0, 32)], keys.at[pl.ds(0, 32)]),
        (k_hbm.at[pl.ds(32, 32)], keys.at[pl.ds(32, 32)]),
        (v_hbm.at[pl.ds(0, 32)], values.at[pl.ds(0, 32)]),
        (v_hbm.at[pl.ds(32, 32)], values.at[pl.ds(32, 32)]),
        (wo_hbm, wo),
        (mlp_gain_hbm, mlp_gain),
        (win_hbm.at[0], win.at[0, pl.ds(0, ff)]),
        (win_hbm.at[1], win.at[1, pl.ds(0, ff)]),
        (wdown_hbm, wdown.at[pl.ds(0, ff)]),
    ]
    copies = [
        pltpu.make_async_copy(src, dst, local_sem.at[at]) for at, (src, dst) in enumerate(pairs)
    ]
    for copy in copies[:3]:
        copy.start()
    barrier = pltpu.get_barrier_semaphore()

    @pl.when(sums & (me < OWNERS))
    def _():
        for offset in ALL:
            for plane in range(C):
                pl.semaphore_signal(
                    barrier, inc=1, device_id=at(kvp_at(*offset), plane), device_id_type=MESH
                )
        pl.semaphore_signal(barrier, inc=1, device_id=at(me, 0), device_id_type=MESH)

    for offset in HEADS:
        pl.semaphore_signal(barrier, inc=1, device_id=head_peer(*offset), device_id_type=MESH)
    for copy in copies[3:]:
        copy.start()

    count, count_ff = 0, 0
    for offset in ALL:
        device = kvp_at(*offset)
        owners[count] = device
        count = count + jnp.where(device < OWNERS, 1, 0)
        candidate = lax.rem(device * UNSPREAD, N)
        tiles[count_ff] = candidate
        count_ff = count_ff + jnp.where(candidate < tiles_ff, 1, 0)

    @pl.when(me < OWNERS)
    def _():
        owners[OWNERS - 1] = me

    @pl.when(my_tile < tiles_ff)
    def _():
        tiles[tiles_ff - 1] = my_tile

    pad = win.shape[1] - ff
    win[:, pl.ds(ff, pad), :] = jnp.zeros((2, pad, win.shape[2]), BF16)
    wdown[pl.ds(ff, pad), :] = jnp.zeros((pad, wdown.shape[1]), BF16)
    turned[...] = jnp.zeros(turned.shape, F32)

    for copy in copies[:3]:
        copy.wait()
    x = hidden[...].astype(F32)
    normed = (x * attn_gain[...][None, :].astype(F32)).astype(BF16)
    partial = jnp.dot(normed, wqkv[...], preferred_element_type=F32)
    for v in range(VECTORS):
        turned[pl.ds(v, B, stride=2 * G), :] = partial[:, v * D : (v + 1) * D]
    square = jnp.sum(x * x, axis=1, keepdims=True)
    high = rounded(square)
    turned[pl.ds(SQUARE_ROW, B, stride=2 * G), :] = jnp.where(
        iota((B, LANES), 1) < LANES // 2, high, square - high
    )
    wide = turned[...].reshape(B, 2 * G, D)
    qkv_send[...] = wide[:, :G].astype(BF16)
    rest_send[...] = wide[:, G : G + REST].astype(BF16)
    pl.semaphore_wait(
        barrier, jnp.where(sums & (me < OWNERS), OWNERS - 1, OWNERS) + len(HEADS)
    )

    def send_qkv(step):
        owner = owners[step]
        copy_to(
            qkv_send.at[owner],
            qkv_recv.at[my_c, me],
            0,
            at(owner, SUMMING),
            sum_sem.at[0, my_c],
        )
        copy_to(
            rest_send.at[owner],
            rest_recv.at[my_c, me],
            13,
            at(owner, SUMMING),
            sum_sem.at[3, my_c],
        )

    for step in range(OWNERS - 1):
        send_qkv(step)

    @pl.when((me >= OWNERS) | (my_c != SUMMING))
    def _():
        send_qkv(OWNERS - 1)

    for copy in copies[3:6]:
        copy.wait()
    sine, cosine = sine_and_cosine(lengths[my_request].astype(F32) * inverse[...])
    lane = iota((G, LANES), 1)
    sine = jnp.where(lane < D // 2, -sine, sine)[0:1]
    cosine = cosine[0:1]
    for copy in copies[6:10]:
        copy.wait()

    @pl.loop(0, keys.shape[0] // TURNS)
    def _(step):
        for turn in range(TURNS):
            keys_across[step * TURNS + turn] = keys[step * TURNS + turn].T

    for copy in copies[11:14]:
        copy.wait()
    for t in range(tiles_ff):
        for part in range(2):
            win_across[t, part] = win[part, pl.ds(t * TILE, LANES), :].T


    def wait_parts(recv_ref, phase, plane):
        arrived = recv_ref.at[plane] if plane != SUMMING else recv_ref.at[plane, pl.ds(0, N - 1)]
        waiter(arrived, 0, sum_sem.at[phase, plane]).wait_recv()

    @pl.when(sums & (me < OWNERS))
    def _():
        qkv_recv[SUMMING, me] = qkv_send[my_request]
        rest_recv[SUMMING, me] = rest_send[my_request]
        for plane in (SUMMING, 1 - SUMMING):
            wait_parts(rest_recv, 3, plane)
            rest = jnp.sum(rest_recv[plane].astype(F32), axis=0)
            square = rest[SQUARE_ROW - G : SQUARE_ROW - G + 1]
            square = square[:, 0:1] + square[:, LANES // 2 : LANES // 2 + 1]
            scale = lax.rsqrt(square / MODEL_WIDTH + EPSILON)
            wait_parts(qkv_recv, 0, plane)
            total = jnp.sum(qkv_recv[plane].astype(F32), axis=0)
            total = jnp.concatenate([total, rest, jnp.zeros_like(rest)], axis=0) * scale
            rotated = total * cosine + pltpu.roll(total, D // 2, 1) * sine
            tile[plane] = jnp.where(iota((2 * G, LANES), 0) <= G, rotated, total).astype(BF16)
            for offset in ALL + [(0, 0)]:
                if offset != (0, 0) or plane != SUMMING:
                    copy_to(
                        tile.at[plane, pl.ds(0, G)],
                        q_all.at[me],
                        1 + plane,
                        at(kvp_at(*offset), plane),
                        query_sem.at[my_z],
                    )
            copy_to(
                tile.at[plane],
                tile.at[plane],
                3 + plane,
                at(kvp_at(Z // 2, 0), SUMMING),
                tile_sem.at[plane],
            )
        q_all[me] = tile[SUMMING, pl.ds(0, G)]

    factor = D ** (-0.5)
    first = me * (PAGES_HERE * PAGE)

    def attend(requests):
        slots = [[table[p, b] for p in range(PAGES_HERE)] for b in requests]
        queries = [q_all[b] for b in requests]
        scores = [
            [
                jnp.dot(query, keys_across[slot], preferred_element_type=F32)
                for slot in here
            ]
            for query, here in zip(queries, slots)
        ]
        parts = []
        for b, here, products in zip(requests, slots, scores):
            left = lengths[b] - first
            live = [lane + p * PAGE < left for p in range(PAGES_HERE)]
            masked = [jnp.where(ok, s * factor, -1e30) for ok, s in zip(live, products)]
            top = jnp.max(functools.reduce(jnp.maximum, masked), axis=1, keepdims=True)
            weights = [jnp.where(ok, jnp.exp(s - top), 0.0) for ok, s in zip(live, masked)]
            total = jnp.sum(functools.reduce(jnp.add, weights), axis=1, keepdims=True)
            summed = 0.0
            for p in range(PAGES_HERE):
                summed = summed + jnp.dot(
                    weights[p].astype(BF16), values[here[p]], preferred_element_type=F32
                )
            high = rounded(top)
            middle = rounded(top - high)
            low = top - high - middle
            stats = jnp.where(
                lane < 32, high, jnp.where(lane < 64, middle, jnp.where(lane < 96, low, total))
            )
            parts.append(jnp.concatenate([summed, stats], axis=0).astype(BF16))
        for b, part in zip(requests, parts):
            part_send[b] = part

    def send_part(request, target):
        copy_to(
            part_send.at[request],
            part_recv.at[my_c, me],
            5,
            at(target, SUMMING),
            sum_sem.at[1, my_c],
        )

    for place in range(ROWS):
        row = 0
        for z in range(Z):
            row = jnp.where(my_z == z, NEAREST_ROWS[z][place], row)
        requests = [row * X + x for x in range(X)]
        if place == 0:

            @pl.when(sums & (me < OWNERS))
            def _(row=row):
                waiter(q_all.at[pl.ds(0, X - 1)], 0, query_sem.at[row]).wait_recv()

            @pl.when(jnp.logical_not(sums & (me < OWNERS)))
            def _(row=row):
                waiter(q_all.at[pl.ds(0, X)], 0, query_sem.at[row]).wait_recv()

        else:
            waiter(q_all.at[pl.ds(0, X)], 0, query_sem.at[row]).wait_recv()
        attend(requests)
        for request in requests:
            for target in (request + OWNERS, request):

                @pl.when((me != target) | (my_c != SUMMING))
                def _(request=request, target=target):
                    send_part(request, target)

    copies[10].wait()

    @pl.when(sums)
    def _():
        part_recv[SUMMING, me] = part_send[my_request]
        for plane in (SUMMING, 1 - SUMMING):

            @pl.when(me >= OWNERS)
            def _(plane=plane):
                waiter(tile.at[plane], 0, tile_sem.at[plane]).wait_recv()

            known = tile[plane].astype(F32)
            new_key, new_value = known[G : G + 1], known[G + 1 : G + 2]
            own = jnp.sum(known[:G] * new_key, axis=1, keepdims=True) * factor
            wait_parts(part_recv, 1, plane)
            tops, overall = [], own
            for k in range(N):
                stats = part_recv[plane, k].astype(F32)[G:]
                tops.append(stats[:, 0:1] + stats[:, 32:33] + stats[:, 64:65])
                overall = jnp.maximum(overall, tops[k])
            own_weight = jnp.exp(own - overall)
            total = own_weight
            summed = rounded(own_weight) * new_value
            for k in range(N):
                part = part_recv[plane, k].astype(F32)
                carried = jnp.exp(tops[k] - overall)
                total = total + part[G:, 96:97] * carried
                summed = summed + part[:G] * carried
            joined[plane] = (summed / total).astype(BF16)
            for offset in NEAR + [(0, 0)]:
                if offset != (0, 0) or plane != SUMMING:
                    copy_to(
                        joined.at[plane],
                        attn_all.at[my_request],
                        6 + plane,
                        at(kvp_at(*offset), plane),
                        all_sem.at[0],
                    )
        attn_all[my_request] = joined[SUMMING]
        waiter(attn_all.at[pl.ds(0, len(NEAR))], 0, all_sem.at[0]).wait_recv()

    @pl.when(my_c != SUMMING)
    def _():
        waiter(attn_all, 0, all_sem.at[0]).wait_recv()

    attn_rows[...] = attn_all[...].astype(F32).reshape(B * G, D)
    attn = jnp.concatenate(
        [attn_rows[pl.ds(g, B, stride=G), :].astype(BF16) for g in range(G)], axis=1
    )

    def over_heads(term, send_ref, recv_ref, phase):
        send_ref[...] = term.astype(BF16)
        for offset in HEADS:
            copy_to(send_ref, recv_ref.at[my_head], phase, head_peer(*offset))
        recv_ref[my_head] = term.astype(BF16)
        waiter(recv_ref.at[pl.ds(0, len(HEADS))], phase).wait_recv()
        return jnp.sum(recv_ref[...].astype(F32), axis=0)

    term = jnp.dot(attn, wo[...], preferred_element_type=F32)
    stream = x + over_heads(term, head_send, head_recv, 8)

    square = jnp.sum(stream * stream, axis=1, keepdims=True)
    high = rounded(square)
    column = iota((B, LANES), 1)
    normed = (stream * mlp_gain[...][None, :].astype(F32)).astype(BF16)
    ours = [tiles[step] for step in range(tiles_ff)]

    def make(step):
        for part in range(2):
            product = jnp.dot(normed, win_across[ours[step], part], preferred_element_type=F32)
            rest = jnp.where(column == TILE, high, square - high) if part == 0 else 0.0
            ff_send[ours[step], part] = jnp.where(column < TILE, product, rest).astype(BF16)

    def send(step):
        copy_to(
            ff_send.at[ours[step]],
            ff_recv.at[my_c, me],
            10,
            at(lax.rem(ours[step] * SPREAD, N), SUMMING),
            sum_sem.at[2, my_c],
        )

    start = 0
    for size in GROUPS:
        for step in range(start, start + size):
            make(step)
        for step in range(start, start + size):
            send(step)
        start += size
    make(start)

    @pl.when((my_tile >= tiles_ff) | (my_c != SUMMING))
    def _():
        send(start)

    summing_tile = sums & (my_tile < tiles_ff)

    @pl.when(summing_tile)
    def _():
        ff_recv[SUMMING, me] = ff_send[my_tile]
        for plane in (SUMMING, 1 - SUMMING):
            wait_parts(ff_recv, 2, plane)
            both = jnp.sum(ff_recv[plane].astype(F32), axis=0)
            square = both[0][:, TILE : TILE + 1] + both[0][:, TILE + 1 : TILE + 2]
            scale = lax.rsqrt(square / MODEL_WIDTH + EPSILON)
            gate, up = both[0] * scale, both[1] * scale
            active = gate / (1.0 + jnp.exp(-gate)) * up
            units[plane] = jnp.where(column < TILE, active, 0.0).astype(BF16)
            for offset in ALL + [(0, 0)]:
                if offset != (0, 0) or plane != SUMMING:
                    copy_to(
                        units.at[plane],
                        hid_all.at[my_tile],
                        11 + plane,
                        at(kvp_at(*offset), plane),
                        all_sem.at[1],
                    )
        hid_all[my_tile] = units[SUMMING]
        waiter(hid_all.at[pl.ds(0, tiles_ff - 1)], 0, all_sem.at[1]).wait_recv()

    @pl.when(jnp.logical_not(summing_tile))
    def _():
        waiter(hid_all, 0, all_sem.at[1]).wait_recv()

    copies[14].wait()
    term = 0.0
    for t in range(tiles_ff):
        term = term + jnp.dot(
            hid_all[t], wdown[pl.ds(t * TILE, LANES), :], preferred_element_type=F32
        )
    out_ref[...] = (stream + over_heads(term, last_send, last_recv, 9)).astype(BF16)

    @pl.when(sums & (me < OWNERS))
    def _():
        waiter(qkv_recv.at[0, pl.ds(0, OWNERS - 1)], 0).wait_send()
        waiter(rest_recv.at[0, pl.ds(0, OWNERS - 1)], 13).wait_send()
        for plane in range(C):
            count = N if plane != SUMMING else N - 1
            waiter(qkv_recv.at[0, pl.ds(0, count)], 1 + plane).wait_send()
            waiter(tile.at[plane], 3 + plane).wait_send()

    @pl.when(jnp.logical_not(sums & (me < OWNERS)))
    def _():
        waiter(qkv_recv.at[0, pl.ds(0, OWNERS)], 0).wait_send()
        waiter(rest_recv.at[0, pl.ds(0, OWNERS)], 13).wait_send()

    @pl.when(sums)
    def _():
        waiter(part_recv.at[0, pl.ds(0, N - 1)], 5).wait_send()
        for plane in range(C):
            count = len(NEAR) + (plane != SUMMING)
            waiter(attn_all.at[pl.ds(0, count)], 6 + plane).wait_send()

    @pl.when(my_c != SUMMING)
    def _():
        waiter(part_recv.at[0], 5).wait_send()

    waiter(head_recv.at[pl.ds(0, len(HEADS))], 8).wait_send()
    waiter(last_recv.at[pl.ds(0, len(HEADS))], 9).wait_send()

    @pl.when(summing_tile)
    def _():
        waiter(ff_recv.at[0, pl.ds(0, tiles_ff - 1)], 10).wait_send()
        for plane in range(C):
            count = N if plane != SUMMING else N - 1
            waiter(part_recv.at[0, pl.ds(0, count)], 11 + plane).wait_send()

    @pl.when(jnp.logical_not(summing_tile))
    def _():
        waiter(ff_recv.at[0, pl.ds(0, tiles_ff)], 10).wait_send()


def on_device(
    hidden_in,
    attn_gain,
    query_key_value_weight,
    k_cache,
    value_cache,
    page_table,
    lengths,
    output_weight,
    mlp_gain,
    w_in,
    w_down,
):
    width = hidden_in.shape[1]
    ff = w_down.shape[0]
    tiles_ff = -(-ff // TILE)
    half = D // 2
    inverse = ROPE_BASE ** (-np.arange(half, dtype=np.float64) * (2.0 / D))
    inverse = np.broadcast_to(np.concatenate([inverse, inverse]), (8, D)).astype(np.float32)
    slots = k_cache.shape[1]
    return pl.pallas_call(
        functools.partial(kernel, tiles_ff, ff),
        out_shape=pltpu.VMEM((B, width), BF16),
        in_specs=[pl.BlockSpec(memory_space=pl.ANY)] * 12,
        out_specs=pl.BlockSpec(memory_space=pltpu.VMEM),
        scratch_shapes=[
            pltpu.VMEM((B, width), BF16),
            pltpu.VMEM((width,), BF16),
            pltpu.VMEM((width,), BF16),
            pltpu.VMEM((8, D), F32),
            pltpu.SMEM((PAGES_HERE, B), jnp.int32),
            pltpu.SMEM((B,), jnp.int32),
            pltpu.VMEM((width, VECTORS * D), BF16),
            pltpu.VMEM((slots, PAGE, D), BF16),
            pltpu.VMEM((slots, PAGE, D), BF16),
            pltpu.VMEM((slots, D, PAGE), BF16),
            pltpu.VMEM((G * D, width), BF16),
            pltpu.VMEM((2, (tiles_ff - 1) * TILE + LANES, width), BF16),
            pltpu.VMEM((tiles_ff, 2, width, LANES), BF16),
            pltpu.VMEM(((tiles_ff - 1) * TILE + LANES, width), BF16),
            pltpu.VMEM((B * 2 * G, D), F32),
            pltpu.VMEM((B, G, D), BF16),
            pltpu.VMEM((C, N, G, D), BF16),
            pltpu.VMEM((B, REST, D), BF16),
            pltpu.VMEM((C, N, REST, D), BF16),
            pltpu.VMEM((B, G, D), BF16),
            pltpu.VMEM((C, 2 * G, D), BF16),
            pltpu.VMEM((B, 2 * G, D), BF16),
            pltpu.VMEM((C, N, 2 * G, D), BF16),
            pltpu.VMEM((C, G, D), BF16),
            pltpu.VMEM((B, G, D), BF16),
            pltpu.VMEM((B * G, D), F32),
            pltpu.VMEM((B, width), BF16),
            pltpu.VMEM((H, B, width), BF16),
            pltpu.VMEM((tiles_ff, 2, B, LANES), BF16),
            pltpu.VMEM((C, N, 2, B, LANES), BF16),
            pltpu.VMEM((C, B, LANES), BF16),
            pltpu.VMEM((tiles_ff, B, LANES), BF16),
            pltpu.VMEM((B, width), BF16),
            pltpu.VMEM((H, B, width), BF16),
            pltpu.SMEM((N,), jnp.int32),
            pltpu.SMEM((N,), jnp.int32),
            pltpu.SemaphoreType.DMA((15,)),
            pltpu.SemaphoreType.DMA((ROWS,)),
            pltpu.SemaphoreType.DMA((4, C)),
            pltpu.SemaphoreType.DMA((C,)),
            pltpu.SemaphoreType.DMA((2,)),
            pltpu.SemaphoreType.DMA((14,)),
            pltpu.SemaphoreType.DMA((14,)),
        ],
        compiler_params=pltpu.CompilerParams(collective_id=0, has_side_effects=True),
    )(
        hidden_in,
        attn_gain,
        query_key_value_weight.transpose(1, 0, 2)[0],
        k_cache[0],
        value_cache[0],
        page_table.T,
        lengths,
        output_weight[0],
        mlp_gain,
        w_in.transpose(1, 2, 0),
        w_down,
        jnp.asarray(inverse),
    )


def solution(mesh):
    return jax.shard_map(
        on_device,
        mesh=mesh,
        in_specs=(
            P(None, "kvp"),
            P("kvp"),
            P("kvp", "head", None),
            P("head", "kvp", None, None),
            P("head", "kvp", None, None),
            P(None, "kvp"),
            P(),
            P("head", None, "kvp"),
            P("kvp"),
            P("kvp", None, "head"),
            P("head", "kvp"),
        ),
        out_specs=P(None, "kvp"),
        check_vma=False,
    )
```

```python
import functools
import math

import jax
import jax.numpy as jnp
import numpy as np
from jax import lax
from jax.experimental import pallas as pl
from jax.experimental.pallas import tpu as pltpu
from jax.sharding import PartitionSpec as P

MESH = pl.DeviceIdType.MESH
F32 = jnp.float32
BF16 = jnp.bfloat16

MODEL_WIDTH = 8192
EPSILON = 1e-05
ROPE_BASE = 10000.0
B = 16
G = 8
D = 128
Z, X = 8, 4
N = Z * X
Y, C = 4, 2
H = Y * C
PAGE = 128
PAGES_HERE = 4
VECTORS = G + 2
LANES = 128
TURNS = 8
TILE = 120
SQUARE_ROW = VECTORS
WIDE = LANES // G
REST = 4
GROUPS = (4, 6, 6, 6)
OWNERS = 16
SUMMING = 1
SPREAD, UNSPREAD = 5, 13


def around(offset, size):
    return min(offset % size, -offset % size)


def far_first(offsets, sizes):
    return sorted(offsets, key=lambda at: -sum(around(o, s) for o, s in zip(at, sizes)))


ALL = far_first([(dz, dx) for dz in range(Z) for dx in range(X) if (dz, dx) != (0, 0)], (Z, X))
NEAR = far_first(
    [(dz, dx) for dz in (-1, 0, 1, 2) for dx in range(X) if (dz, dx) != (0, 0)], (Z, X)
)
HEADS = far_first([(dy, dc) for dy in range(Y) for dc in range(C) if (dy, dc) != (0, 0)], (Y, C))


ROWS = OWNERS // X
NEAREST_ROWS = [sorted(range(ROWS), key=lambda row: around(row - z, Z)) for z in range(Z)]


def iota(shape, dim):
    return lax.broadcasted_iota(jnp.int32, shape, dim)


def rounded(value):
    return value.astype(BF16).astype(F32)


def sine_and_cosine(angle):
    turns = jnp.floor(angle * (1.0 / (2.0 * math.pi)) + 0.5)
    left = angle - turns * 6.28125
    left = left - turns * (2.0 * math.pi - 6.28125)
    y = left * 0.5
    z = y * y
    sine, cosine = 0.0, 0.0
    for k in range(6, -1, -1):
        sine = sine * z + (-1.0) ** k / math.factorial(2 * k + 1)
    sine = sine * y
    for k in range(7, -1, -1):
        cosine = cosine * z + (-1.0) ** k / math.factorial(2 * k)
    return 2.0 * sine * cosine, 1.0 - 2.0 * sine * sine


def kernel(
    tiles_ff,
    ff,
    hidden_hbm,
    attn_gain_hbm,
    qkv_hbm,
    k_hbm,
    v_hbm,
    table_hbm,
    lengths_hbm,
    wo_hbm,
    mlp_gain_hbm,
    win_hbm,
    wdown_hbm,
    inverse_hbm,
    out_ref,
    hidden,
    attn_gain,
    mlp_gain,
    inverse,
    table,
    lengths,
    wqkv,
    keys,
    values,
    keys_across,
    wo,
    win,
    win_across,
    wdown,
    turned,
    qkv_send,
    qkv_recv,
    rest_send,
    rest_recv,
    q_all,
    tile_out,
    tile,
    part_send,
    part_recv,
    stat_send,
    stat_recv,
    joined,
    attn_all,
    attn_rows,
    head_send,
    head_recv,
    ff_send,
    ff_recv,
    units,
    hid_all,
    last_send,
    last_recv,
    owners,
    tiles,
    local_sem,
    query_sem,
    sum_sem,
    tile_sem,
    all_sem,
    send_sem,
    recv_sem,
):
    me = lax.axis_index("kvp")
    my_head = lax.axis_index("head")
    my_z, my_x = me // X, lax.rem(me, X)
    my_y, my_c = my_head // C, lax.rem(my_head, C)
    zs = [lax.rem(my_z + dz, Z) for dz in range(Z)]
    xs = [lax.rem(my_x + dx, X) for dx in range(X)]
    ys = [lax.rem(my_y + dy, Y) for dy in range(Y)]
    cs = [lax.rem(my_c + dc, C) for dc in range(C)]

    sums = my_c == SUMMING

    def at(kvp, plane):
        return {"kvp": kvp, "head": my_y * C + plane}

    def kvp_at(dz, dx):
        return zs[dz % Z] * X + xs[dx % X]

    def head_peer(dy, dc):
        return {"head": ys[dy] * C + cs[dc]}

    request_of_z = [lax.rem(z + Z // 4, Z // 2) * X for z in zs]

    def request_at(dz, dx):
        return request_of_z[dz % Z] + xs[dx % X]

    my_request = request_at(0, 0)

    def joiners(request):
        return lax.rem(request + 3 * N // 4, N), request + N // 4

    my_tile = lax.rem(me * UNSPREAD, N)

    def copy_to(src, dst, phase, device, arrival=None):
        pltpu.make_async_remote_copy(
            src_ref=src,
            dst_ref=dst,
            send_sem=send_sem.at[phase],
            recv_sem=recv_sem.at[phase] if arrival is None else arrival,
            device_id=device,
            device_id_type=MESH,
        ).start()

    def waiter(ref, phase, arrival=None):
        return pltpu.make_async_remote_copy(
            src_ref=ref,
            dst_ref=ref,
            send_sem=send_sem.at[phase],
            recv_sem=recv_sem.at[phase] if arrival is None else arrival,
            device_id={"kvp": kvp_at(1, 0)},
            device_id_type=MESH,
        )

    pairs = [
        (hidden_hbm, hidden),
        (attn_gain_hbm, attn_gain),
        (qkv_hbm, wqkv),
        (lengths_hbm, lengths),
        (inverse_hbm, inverse),
        (table_hbm, table),
        (k_hbm.at[pl.ds(0, 32)], keys.at[pl.ds(0, 32)]),
        (k_hbm.at[pl.ds(32, 32)], keys.at[pl.ds(32, 32)]),
        (v_hbm.at[pl.ds(0, 32)], values.at[pl.ds(0, 32)]),
        (v_hbm.at[pl.ds(32, 32)], values.at[pl.ds(32, 32)]),
        (wo_hbm, wo),
        (mlp_gain_hbm, mlp_gain),
        (win_hbm.at[0], win.at[0, pl.ds(0, ff)]),
        (win_hbm.at[1], win.at[1, pl.ds(0, ff)]),
        (wdown_hbm, wdown.at[pl.ds(0, ff)]),
    ]
    copies = [
        pltpu.make_async_copy(src, dst, local_sem.at[at]) for at, (src, dst) in enumerate(pairs)
    ]
    for copy in copies[:3]:
        copy.start()
    barrier = pltpu.get_barrier_semaphore()

    @pl.when(sums & (me < OWNERS))
    def _():
        for offset in ALL:
            for plane in range(C):
                pl.semaphore_signal(
                    barrier, inc=1, device_id=at(kvp_at(*offset), plane), device_id_type=MESH
                )
        pl.semaphore_signal(barrier, inc=1, device_id=at(me, 0), device_id_type=MESH)

    for offset in HEADS:
        pl.semaphore_signal(barrier, inc=1, device_id=head_peer(*offset), device_id_type=MESH)
    for copy in copies[3:]:
        copy.start()

    count, count_ff = 0, 0
    for offset in ALL:
        device = kvp_at(*offset)
        owners[count] = device
        count = count + jnp.where(device < OWNERS, 1, 0)
        candidate = lax.rem(device * UNSPREAD, N)
        tiles[count_ff] = candidate
        count_ff = count_ff + jnp.where(candidate < tiles_ff, 1, 0)

    @pl.when(me < OWNERS)
    def _():
        owners[OWNERS - 1] = me

    @pl.when(my_tile < tiles_ff)
    def _():
        tiles[tiles_ff - 1] = my_tile

    pad = win.shape[1] - ff
    win[:, pl.ds(ff, pad), :] = jnp.zeros((2, pad, win.shape[2]), BF16)
    wdown[pl.ds(ff, pad), :] = jnp.zeros((pad, wdown.shape[1]), BF16)
    turned[...] = jnp.zeros(turned.shape, F32)

    for copy in copies[:3]:
        copy.wait()
    x = hidden[...].astype(F32)
    normed = (x * attn_gain[...][None, :].astype(F32)).astype(BF16)
    partial = jnp.dot(normed, wqkv[...], preferred_element_type=F32)
    for v in range(VECTORS):
        turned[pl.ds(v, B, stride=2 * G), :] = partial[:, v * D : (v + 1) * D]
    square = jnp.sum(x * x, axis=1, keepdims=True)
    high = rounded(square)
    turned[pl.ds(SQUARE_ROW, B, stride=2 * G), :] = jnp.where(
        iota((B, LANES), 1) < LANES // 2, high, square - high
    )
    wide = turned[...].reshape(B, 2 * G, D)
    qkv_send[...] = wide[:, :G].astype(BF16)
    rest_send[...] = wide[:, G : G + REST].astype(BF16)
    pl.semaphore_wait(
        barrier, jnp.where(sums & (me < OWNERS), OWNERS - 1, OWNERS) + len(HEADS)
    )

    def send_qkv(step):
        owner = owners[step]
        copy_to(
            qkv_send.at[owner],
            qkv_recv.at[my_c, me],
            0,
            at(owner, SUMMING),
            sum_sem.at[0, my_c],
        )
        copy_to(
            rest_send.at[owner],
            rest_recv.at[my_c, me],
            13,
            at(owner, SUMMING),
            sum_sem.at[3, my_c],
        )

    for step in range(OWNERS - 1):
        send_qkv(step)

    @pl.when((me >= OWNERS) | (my_c != SUMMING))
    def _():
        send_qkv(OWNERS - 1)

    for copy in copies[3:6]:
        copy.wait()
    sine, cosine = sine_and_cosine(lengths[lax.rem(me, OWNERS)].astype(F32) * inverse[...])
    lane = iota((G, LANES), 1)
    sine = jnp.where(lane < D // 2, -sine, sine)[0:1]
    cosine = cosine[0:1]
    for copy in copies[6:10]:
        copy.wait()

    @pl.loop(0, keys.shape[0] // TURNS)
    def _(step):
        for turn in range(TURNS):
            keys_across[step * TURNS + turn] = keys[step * TURNS + turn].T

    for copy in copies[11:14]:
        copy.wait()
    for t in range(tiles_ff):
        for part in range(2):
            win_across[t, part] = win[part, pl.ds(t * TILE, LANES), :].T


    def wait_parts(recv_ref, phase, plane):
        arrived = recv_ref.at[plane] if plane != SUMMING else recv_ref.at[plane, pl.ds(0, N - 1)]
        waiter(arrived, 0, sum_sem.at[phase, plane]).wait_recv()

    @pl.when(sums & (me < OWNERS))
    def _():
        qkv_recv[SUMMING, me] = qkv_send[me]
        rest_recv[SUMMING, me] = rest_send[me]
        for plane in (SUMMING, 1 - SUMMING):
            wait_parts(rest_recv, 3, plane)
            rest = jnp.sum(rest_recv[plane].astype(F32), axis=0)
            square = rest[SQUARE_ROW - G : SQUARE_ROW - G + 1]
            square = square[:, 0:1] + square[:, LANES // 2 : LANES // 2 + 1]
            scale = lax.rsqrt(square / MODEL_WIDTH + EPSILON)
            wait_parts(qkv_recv, 0, plane)
            total = jnp.sum(qkv_recv[plane].astype(F32), axis=0)
            total = jnp.concatenate([total, rest, jnp.zeros_like(rest)], axis=0) * scale
            rotated = total * cosine + pltpu.roll(total, D // 2, 1) * sine
            tile_out[plane] = jnp.where(iota((2 * G, LANES), 0) <= G, rotated, total).astype(BF16)
            for offset in ALL + [(0, 0)]:
                if offset != (0, 0) or plane != SUMMING:
                    copy_to(
                        tile_out.at[plane, pl.ds(0, G)],
                        q_all.at[me],
                        1 + plane,
                        at(kvp_at(*offset), plane),
                        query_sem.at[my_z],
                    )
            for target in joiners(me):
                copy_to(
                    tile_out.at[plane],
                    tile.at[plane],
                    3 + plane,
                    at(target, SUMMING),
                    tile_sem.at[plane],
                )
        q_all[me] = tile_out[SUMMING, pl.ds(0, G)]

    head_at = iota((G, LANES), 0) * WIDE
    in_block = (lane >= head_at) & (lane < head_at + WIDE)

    def to_column(row):
        return jnp.sum(jnp.where(lane == head_at, row, 0.0), axis=1, keepdims=True)

    factor = D ** (-0.5)
    first = me * (PAGES_HERE * PAGE)

    def attend(requests):
        slots = [[table[p, b] for p in range(PAGES_HERE)] for b in requests]
        queries = [q_all[b] for b in requests]
        scores = [
            [
                jnp.dot(query, keys_across[slot], preferred_element_type=F32)
                for slot in here
            ]
            for query, here in zip(queries, slots)
        ]
        parts = []
        for b, here, products in zip(requests, slots, scores):
            left = lengths[b] - first
            live = [lane + p * PAGE < left for p in range(PAGES_HERE)]
            masked = [jnp.where(ok, s * factor, -1e30) for ok, s in zip(live, products)]
            top = jnp.max(functools.reduce(jnp.maximum, masked), axis=1, keepdims=True)
            weights = [jnp.where(ok, jnp.exp(s - top), 0.0) for ok, s in zip(live, masked)]
            total = jnp.sum(functools.reduce(jnp.add, weights), axis=1, keepdims=True)
            summed = 0.0
            for p in range(PAGES_HERE):
                summed = summed + jnp.dot(
                    weights[p].astype(BF16), values[here[p]], preferred_element_type=F32
                )
            both = jnp.where(lane % WIDE < WIDE // 2, top, total)
            row = jnp.sum(jnp.where(in_block, both, 0.0), axis=0, keepdims=True)
            parts.append((summed.astype(BF16), row))
        for b, (part, row) in zip(requests, parts):
            part_send[b] = part
            stat_send[b] = row

    def send_part(request, target):
        copy_to(
            part_send.at[request],
            part_recv.at[my_c, me],
            5,
            at(target, SUMMING),
            sum_sem.at[1, my_c],
        )
        copy_to(
            stat_send.at[request],
            stat_recv.at[my_c, pl.ds(me, 1)],
            14,
            at(target, SUMMING),
            sum_sem.at[4, my_c],
        )

    for place in range(ROWS):
        row = 0
        for z in range(Z):
            row = jnp.where(my_z == z, NEAREST_ROWS[z][place], row)
        requests = [row * X + x for x in range(X)]
        if place == 0:

            @pl.when(sums & (me < OWNERS))
            def _(row=row):
                waiter(q_all.at[pl.ds(0, X - 1)], 0, query_sem.at[row]).wait_recv()

            @pl.when(jnp.logical_not(sums & (me < OWNERS)))
            def _(row=row):
                waiter(q_all.at[pl.ds(0, X)], 0, query_sem.at[row]).wait_recv()

        else:
            waiter(q_all.at[pl.ds(0, X)], 0, query_sem.at[row]).wait_recv()
        attend(requests)
        for request in requests:
            for target in joiners(request):

                @pl.when((me != target) | (my_c != SUMMING))
                def _(request=request, target=target):
                    send_part(request, target)

    copies[10].wait()

    @pl.when(sums)
    def _():
        part_recv[SUMMING, me] = part_send[my_request]
        stat_recv[SUMMING, pl.ds(me, 1)] = stat_send[my_request]
        for plane in (SUMMING, 1 - SUMMING):

            waiter(tile.at[plane], 0, tile_sem.at[plane]).wait_recv()
            known = tile[plane].astype(F32)
            new_key, new_value = known[G : G + 1], known[G + 1 : G + 2]
            own = jnp.sum(known[:G] * new_key, axis=1, keepdims=True) * factor
            own_row = jnp.sum(jnp.where(in_block, own, 0.0), axis=0, keepdims=True)
            wait_parts(stat_recv, 4, plane)
            stats = stat_recv[plane]
            overall = jnp.maximum(jnp.max(stats, axis=0, keepdims=True), own_row)
            carried = jnp.exp(stats - overall)
            totals = pltpu.roll(stats, LANES - WIDE // 2, 1)
            own_row = jnp.exp(own_row - overall)
            total = to_column(jnp.sum(totals * carried, axis=0, keepdims=True) + own_row)
            summed = rounded(to_column(own_row)) * new_value
            carried = [to_column(carried[k : k + 1]) for k in range(N)]
            wait_parts(part_recv, 1, plane)
            for k in range(N):
                summed = summed + part_recv[plane, k].astype(F32) * carried[k]
            joined[plane] = (summed / total).astype(BF16)
            for offset in NEAR + [(0, 0)]:
                if offset != (0, 0) or plane != SUMMING:
                    copy_to(
                        joined.at[plane],
                        attn_all.at[my_request],
                        6 + plane,
                        at(kvp_at(*offset), plane),
                        all_sem.at[0],
                    )
        attn_all[my_request] = joined[SUMMING]
        waiter(attn_all.at[pl.ds(0, len(NEAR))], 0, all_sem.at[0]).wait_recv()

    @pl.when(my_c != SUMMING)
    def _():
        waiter(attn_all, 0, all_sem.at[0]).wait_recv()

    attn_rows[...] = attn_all[...].astype(F32).reshape(B * G, D)
    attn = jnp.concatenate(
        [attn_rows[pl.ds(g, B, stride=G), :].astype(BF16) for g in range(G)], axis=1
    )

    def over_heads(term, send_ref, recv_ref, phase):
        send_ref[...] = term.astype(BF16)
        for offset in HEADS:
            copy_to(send_ref, recv_ref.at[my_head], phase, head_peer(*offset))
        recv_ref[my_head] = term.astype(BF16)
        waiter(recv_ref.at[pl.ds(0, len(HEADS))], phase).wait_recv()
        return jnp.sum(recv_ref[...].astype(F32), axis=0)

    term = jnp.dot(attn, wo[...], preferred_element_type=F32)
    stream = x + over_heads(term, head_send, head_recv, 8)

    square = jnp.sum(stream * stream, axis=1, keepdims=True)
    high = rounded(square)
    column = iota((B, LANES), 1)
    normed = (stream * mlp_gain[...][None, :].astype(F32)).astype(BF16)
    ours = [tiles[step] for step in range(tiles_ff)]

    def make(step):
        for part in range(2):
            product = jnp.dot(normed, win_across[ours[step], part], preferred_element_type=F32)
            rest = jnp.where(column == TILE, high, square - high) if part == 0 else 0.0
            ff_send[ours[step], part] = jnp.where(column < TILE, product, rest).astype(BF16)

    def send(step):
        copy_to(
            ff_send.at[ours[step]],
            ff_recv.at[my_c, me],
            10,
            at(lax.rem(ours[step] * SPREAD, N), SUMMING),
            sum_sem.at[2, my_c],
        )

    start = 0
    for size in GROUPS:
        for step in range(start, start + size):
            make(step)
        for step in range(start, start + size):
            send(step)
        start += size
    make(start)

    @pl.when((my_tile >= tiles_ff) | (my_c != SUMMING))
    def _():
        send(start)

    summing_tile = sums & (my_tile < tiles_ff)

    @pl.when(summing_tile)
    def _():
        ff_recv[SUMMING, me] = ff_send[my_tile]
        for plane in (SUMMING, 1 - SUMMING):
            wait_parts(ff_recv, 2, plane)
            both = jnp.sum(ff_recv[plane].astype(F32), axis=0)
            square = both[0][:, TILE : TILE + 1] + both[0][:, TILE + 1 : TILE + 2]
            scale = lax.rsqrt(square / MODEL_WIDTH + EPSILON)
            gate, up = both[0] * scale, both[1] * scale
            active = gate / (1.0 + jnp.exp(-gate)) * up
            units[plane] = jnp.where(column < TILE, active, 0.0).astype(BF16)
            for offset in ALL + [(0, 0)]:
                if offset != (0, 0) or plane != SUMMING:
                    copy_to(
                        units.at[plane],
                        hid_all.at[my_tile],
                        11 + plane,
                        at(kvp_at(*offset), plane),
                        all_sem.at[1],
                    )
        hid_all[my_tile] = units[SUMMING]
        waiter(hid_all.at[pl.ds(0, tiles_ff - 1)], 0, all_sem.at[1]).wait_recv()

    @pl.when(jnp.logical_not(summing_tile))
    def _():
        waiter(hid_all, 0, all_sem.at[1]).wait_recv()

    copies[14].wait()
    term = 0.0
    for t in range(tiles_ff):
        term = term + jnp.dot(
            hid_all[t], wdown[pl.ds(t * TILE, LANES), :], preferred_element_type=F32
        )
    out_ref[...] = (stream + over_heads(term, last_send, last_recv, 9)).astype(BF16)

    @pl.when(sums & (me < OWNERS))
    def _():
        waiter(qkv_recv.at[0, pl.ds(0, OWNERS - 1)], 0).wait_send()
        waiter(rest_recv.at[0, pl.ds(0, OWNERS - 1)], 13).wait_send()
        for plane in range(C):
            count = N if plane != SUMMING else N - 1
            waiter(qkv_recv.at[0, pl.ds(0, count)], 1 + plane).wait_send()
            waiter(tile_out, 3 + plane).wait_send()

    @pl.when(jnp.logical_not(sums & (me < OWNERS)))
    def _():
        waiter(qkv_recv.at[0, pl.ds(0, OWNERS)], 0).wait_send()
        waiter(rest_recv.at[0, pl.ds(0, OWNERS)], 13).wait_send()

    @pl.when(sums)
    def _():
        waiter(part_recv.at[0, pl.ds(0, N - 1)], 5).wait_send()
        waiter(stat_recv.at[0, pl.ds(0, N - 1)], 14).wait_send()
        for plane in range(C):
            count = len(NEAR) + (plane != SUMMING)
            waiter(attn_all.at[pl.ds(0, count)], 6 + plane).wait_send()

    @pl.when(my_c != SUMMING)
    def _():
        waiter(part_recv.at[0], 5).wait_send()
        waiter(stat_recv.at[0], 14).wait_send()

    waiter(head_recv.at[pl.ds(0, len(HEADS))], 8).wait_send()
    waiter(last_recv.at[pl.ds(0, len(HEADS))], 9).wait_send()

    @pl.when(summing_tile)
    def _():
        waiter(ff_recv.at[0, pl.ds(0, tiles_ff - 1)], 10).wait_send()
        for plane in range(C):
            count = N if plane != SUMMING else N - 1
            waiter(ff_recv.at[0, pl.ds(0, count), 0], 11 + plane).wait_send()

    @pl.when(jnp.logical_not(summing_tile))
    def _():
        waiter(ff_recv.at[0, pl.ds(0, tiles_ff)], 10).wait_send()


def on_device(
    hidden_in,
    attn_gain,
    query_key_value_weight,
    k_cache,
    value_cache,
    page_table,
    lengths,
    output_weight,
    mlp_gain,
    w_in,
    w_down,
):
    width = hidden_in.shape[1]
    ff = w_down.shape[0]
    tiles_ff = -(-ff // TILE)
    half = D // 2
    inverse = ROPE_BASE ** (-np.arange(half, dtype=np.float64) * (2.0 / D))
    inverse = np.broadcast_to(np.concatenate([inverse, inverse]), (8, D)).astype(np.float32)
    slots = k_cache.shape[1]
    return pl.pallas_call(
        functools.partial(kernel, tiles_ff, ff),
        out_shape=pltpu.VMEM((B, width), BF16),
        in_specs=[pl.BlockSpec(memory_space=pl.ANY)] * 12,
        out_specs=pl.BlockSpec(memory_space=pltpu.VMEM),
        scratch_shapes=[
            pltpu.VMEM((B, width), BF16),
            pltpu.VMEM((width,), BF16),
            pltpu.VMEM((width,), BF16),
            pltpu.VMEM((8, D), F32),
            pltpu.SMEM((PAGES_HERE, B), jnp.int32),
            pltpu.SMEM((B,), jnp.int32),
            pltpu.VMEM((width, VECTORS * D), BF16),
            pltpu.VMEM((slots, PAGE, D), BF16),
            pltpu.VMEM((slots, PAGE, D), BF16),
            pltpu.VMEM((slots, D, PAGE), BF16),
            pltpu.VMEM((G * D, width), BF16),
            pltpu.VMEM((2, (tiles_ff - 1) * TILE + LANES, width), BF16),
            pltpu.VMEM((tiles_ff, 2, width, LANES), BF16),
            pltpu.VMEM(((tiles_ff - 1) * TILE + LANES, width), BF16),
            pltpu.VMEM((B * 2 * G, D), F32),
            pltpu.VMEM((B, G, D), BF16),
            pltpu.VMEM((C, N, G, D), BF16),
            pltpu.VMEM((B, REST, D), BF16),
            pltpu.VMEM((C, N, REST, D), BF16),
            pltpu.VMEM((B, G, D), BF16),
            pltpu.VMEM((C, 2 * G, D), BF16),
            pltpu.VMEM((C, 2 * G, D), BF16),
            pltpu.VMEM((B, G, D), BF16),
            pltpu.VMEM((C, N, G, D), BF16),
            pltpu.VMEM((B, 1, LANES), F32),
            pltpu.VMEM((C, N, LANES), F32),
            pltpu.VMEM((C, G, D), BF16),
            pltpu.VMEM((B, G, D), BF16),
            pltpu.VMEM((B * G, D), F32),
            pltpu.VMEM((B, width), BF16),
            pltpu.VMEM((H, B, width), BF16),
            pltpu.VMEM((tiles_ff, 2, B, LANES), BF16),
            pltpu.VMEM((C, N, 2, B, LANES), BF16),
            pltpu.VMEM((C, B, LANES), BF16),
            pltpu.VMEM((tiles_ff, B, LANES), BF16),
            pltpu.VMEM((B, width), BF16),
            pltpu.VMEM((H, B, width), BF16),
            pltpu.SMEM((N,), jnp.int32),
            pltpu.SMEM((N,), jnp.int32),
            pltpu.SemaphoreType.DMA((15,)),
            pltpu.SemaphoreType.DMA((ROWS,)),
            pltpu.SemaphoreType.DMA((5, C)),
            pltpu.SemaphoreType.DMA((C,)),
            pltpu.SemaphoreType.DMA((2,)),
            pltpu.SemaphoreType.DMA((15,)),
            pltpu.SemaphoreType.DMA((15,)),
        ],
        compiler_params=pltpu.CompilerParams(collective_id=0, has_side_effects=True),
    )(
        hidden_in,
        attn_gain,
        query_key_value_weight.transpose(1, 0, 2)[0],
        k_cache[0],
        value_cache[0],
        page_table.T,
        lengths,
        output_weight[0],
        mlp_gain,
        w_in.transpose(1, 2, 0),
        w_down,
        jnp.asarray(inverse),
    )


def solution(mesh):
    return jax.shard_map(
        on_device,
        mesh=mesh,
        in_specs=(
            P(None, "kvp"),
            P("kvp"),
            P("kvp", "head", None),
            P("head", "kvp", None, None),
            P("head", "kvp", None, None),
            P(None, "kvp"),
            P(),
            P("head", None, "kvp"),
            P("kvp"),
            P("kvp", None, "head"),
            P("head", "kvp"),
        ),
        out_specs=P(None, "kvp"),
        check_vma=False,
    )
```

```python
import functools
import math

import jax
import jax.numpy as jnp
import numpy as np
from jax import lax
from jax.experimental import pallas as pl
from jax.experimental.pallas import tpu as pltpu
from jax.sharding import PartitionSpec as P

MESH = pl.DeviceIdType.MESH
F32 = jnp.float32
BF16 = jnp.bfloat16

MODEL_WIDTH = 8192
EPSILON = 1e-05
ROPE_BASE = 10000.0
B = 16
G = 8
D = 128
Z, X = 8, 4
N = Z * X
Y, C = 4, 2
H = Y * C
PAGE = 128
PAGES_HERE = 4
VECTORS = G + 2
LANES = 128
TURNS = 8
TILE = 120
SQUARE_ROW = VECTORS
WIDE = LANES // G
REST = 4
GROUPS = (4, 6, 6, 6)
OWNERS = 16
SUMMING = 1
SPREAD, UNSPREAD = 5, 13


def around(offset, size):
    return min(offset % size, -offset % size)


def far_first(offsets, sizes):
    return sorted(
        offsets,
        key=lambda at: (-sum(around(o, s) for o, s in zip(at, sizes)), -around(at[0], sizes[0])),
    )


ALL = far_first([(dz, dx) for dz in range(Z) for dx in range(X) if (dz, dx) != (0, 0)], (Z, X))
NEAR = far_first(
    [(dz, dx) for dz in (-1, 0, 1, 2) for dx in range(X) if (dz, dx) != (0, 0)], (Z, X)
)
HEADS = far_first([(dy, dc) for dy in range(Y) for dc in range(C) if (dy, dc) != (0, 0)], (Y, C))


ROWS = OWNERS // X
NEAREST_ROWS = [sorted(range(ROWS), key=lambda row: around(row - z, Z)) for z in range(Z)]


def iota(shape, dim):
    return lax.broadcasted_iota(jnp.int32, shape, dim)


def rounded(value):
    return value.astype(BF16).astype(F32)


def sine_and_cosine(angle):
    turns = jnp.floor(angle * (1.0 / (2.0 * math.pi)) + 0.5)
    left = angle - turns * 6.28125
    left = left - turns * (2.0 * math.pi - 6.28125)
    y = left * 0.5
    z = y * y
    sine, cosine = 0.0, 0.0
    for k in range(6, -1, -1):
        sine = sine * z + (-1.0) ** k / math.factorial(2 * k + 1)
    sine = sine * y
    for k in range(7, -1, -1):
        cosine = cosine * z + (-1.0) ** k / math.factorial(2 * k)
    return 2.0 * sine * cosine, 1.0 - 2.0 * sine * sine


def kernel(
    tiles_ff,
    ff,
    hidden_hbm,
    attn_gain_hbm,
    qkv_hbm,
    k_hbm,
    v_hbm,
    table_hbm,
    lengths_hbm,
    wo_hbm,
    mlp_gain_hbm,
    win_hbm,
    wdown_hbm,
    inverse_hbm,
    out_ref,
    hidden,
    attn_gain,
    mlp_gain,
    inverse,
    table,
    lengths,
    wqkv,
    keys,
    values,
    keys_across,
    wo,
    win,
    win_across,
    wdown,
    turned,
    qkv_send,
    qkv_recv,
    rest_send,
    rest_recv,
    q_all,
    tile_out,
    tile,
    part_send,
    part_recv,
    stat_send,
    stat_recv,
    joined,
    attn_all,
    attn_rows,
    head_send,
    head_recv,
    ff_send,
    ff_recv,
    units,
    hid_all,
    last_send,
    last_recv,
    owners,
    tiles,
    local_sem,
    query_sem,
    sum_sem,
    tile_sem,
    all_sem,
    send_sem,
    recv_sem,
):
    me = lax.axis_index("kvp")
    my_head = lax.axis_index("head")
    my_z, my_x = me // X, lax.rem(me, X)
    my_y, my_c = my_head // C, lax.rem(my_head, C)
    zs = [lax.rem(my_z + dz, Z) for dz in range(Z)]
    xs = [lax.rem(my_x + dx, X) for dx in range(X)]
    ys = [lax.rem(my_y + dy, Y) for dy in range(Y)]
    cs = [lax.rem(my_c + dc, C) for dc in range(C)]

    sums = my_c == SUMMING

    def at(kvp, plane):
        return {"kvp": kvp, "head": my_y * C + plane}

    def kvp_at(dz, dx):
        return zs[dz % Z] * X + xs[dx % X]

    def head_peer(dy, dc):
        return {"head": ys[dy] * C + cs[dc]}

    request_of_z = [lax.rem(z + Z // 4, Z // 2) * X for z in zs]

    def request_at(dz, dx):
        return request_of_z[dz % Z] + xs[dx % X]

    my_request = request_at(0, 0)

    def joiners(request):
        return lax.rem(request + 3 * N // 4, N), request + N // 4

    my_tile = lax.rem(me * UNSPREAD, N)

    def copy_to(src, dst, phase, device, arrival=None):
        pltpu.make_async_remote_copy(
            src_ref=src,
            dst_ref=dst,
            send_sem=send_sem.at[phase],
            recv_sem=recv_sem.at[phase] if arrival is None else arrival,
            device_id=device,
            device_id_type=MESH,
        ).start()

    def waiter(ref, phase, arrival=None):
        return pltpu.make_async_remote_copy(
            src_ref=ref,
            dst_ref=ref,
            send_sem=send_sem.at[phase],
            recv_sem=recv_sem.at[phase] if arrival is None else arrival,
            device_id={"kvp": kvp_at(1, 0)},
            device_id_type=MESH,
        )

    pairs = [
        (hidden_hbm, hidden),
        (attn_gain_hbm, attn_gain),
        (qkv_hbm, wqkv),
        (lengths_hbm, lengths),
        (inverse_hbm, inverse),
        (table_hbm, table),
        (k_hbm.at[pl.ds(0, 32)], keys.at[pl.ds(0, 32)]),
        (k_hbm.at[pl.ds(32, 32)], keys.at[pl.ds(32, 32)]),
        (v_hbm.at[pl.ds(0, 32)], values.at[pl.ds(0, 32)]),
        (v_hbm.at[pl.ds(32, 32)], values.at[pl.ds(32, 32)]),
        (wo_hbm, wo),
        (mlp_gain_hbm, mlp_gain),
        (win_hbm.at[0], win.at[0, pl.ds(0, ff)]),
        (win_hbm.at[1], win.at[1, pl.ds(0, ff)]),
        (wdown_hbm, wdown.at[pl.ds(0, ff)]),
    ]
    copies = [
        pltpu.make_async_copy(src, dst, local_sem.at[at]) for at, (src, dst) in enumerate(pairs)
    ]
    for copy in copies[:3]:
        copy.start()
    barrier = pltpu.get_barrier_semaphore()

    @pl.when(sums & (me < OWNERS))
    def _():
        for offset in ALL:
            for plane in range(C):
                pl.semaphore_signal(
                    barrier, inc=1, device_id=at(kvp_at(*offset), plane), device_id_type=MESH
                )
        pl.semaphore_signal(barrier, inc=1, device_id=at(me, 0), device_id_type=MESH)

    for offset in HEADS:
        pl.semaphore_signal(barrier, inc=1, device_id=head_peer(*offset), device_id_type=MESH)
    for copy in copies[3:]:
        copy.start()

    count, count_ff = 0, 0
    for offset in ALL:
        device = kvp_at(*offset)
        owners[count] = device
        count = count + jnp.where(device < OWNERS, 1, 0)
        candidate = lax.rem(device * UNSPREAD, N)
        tiles[count_ff] = candidate
        count_ff = count_ff + jnp.where(candidate < tiles_ff, 1, 0)

    @pl.when(me < OWNERS)
    def _():
        owners[OWNERS - 1] = me

    @pl.when(my_tile < tiles_ff)
    def _():
        tiles[tiles_ff - 1] = my_tile

    pad = win.shape[1] - ff
    win[:, pl.ds(ff, pad), :] = jnp.zeros((2, pad, win.shape[2]), BF16)
    wdown[pl.ds(ff, pad), :] = jnp.zeros((pad, wdown.shape[1]), BF16)
    turned[...] = jnp.zeros(turned.shape, F32)

    for copy in copies[:3]:
        copy.wait()
    x = hidden[...].astype(F32)
    normed = (x * attn_gain[...][None, :].astype(F32)).astype(BF16)
    partial = jnp.dot(normed, wqkv[...], preferred_element_type=F32)
    for v in range(VECTORS):
        turned[pl.ds(v, B, stride=2 * G), :] = partial[:, v * D : (v + 1) * D]
    square = jnp.sum(x * x, axis=1, keepdims=True)
    high = rounded(square)
    turned[pl.ds(SQUARE_ROW, B, stride=2 * G), :] = jnp.where(
        iota((B, LANES), 1) < LANES // 2, high, square - high
    )
    wide = turned[...].reshape(B, 2 * G, D)
    qkv_send[...] = wide[:, :G].astype(BF16)
    rest_send[...] = wide[:, G : G + REST].astype(BF16)
    pl.semaphore_wait(
        barrier, jnp.where(sums & (me < OWNERS), OWNERS - 1, OWNERS) + len(HEADS)
    )

    def send_qkv(step):
        owner = owners[step]
        copy_to(
            qkv_send.at[owner],
            qkv_recv.at[my_c, me],
            0,
            at(owner, SUMMING),
            sum_sem.at[0, my_c],
        )
        copy_to(
            rest_send.at[owner],
            rest_recv.at[my_c, me],
            13,
            at(owner, SUMMING),
            sum_sem.at[3, my_c],
        )

    for step in range(OWNERS - 1):
        send_qkv(step)

    @pl.when((me >= OWNERS) | (my_c != SUMMING))
    def _():
        send_qkv(OWNERS - 1)

    for copy in copies[3:6]:
        copy.wait()
    sine, cosine = sine_and_cosine(lengths[lax.rem(me, OWNERS)].astype(F32) * inverse[...])
    lane = iota((G, LANES), 1)
    sine = jnp.where(lane < D // 2, -sine, sine)[0:1]
    cosine = cosine[0:1]
    for copy in copies[6:10]:
        copy.wait()

    @pl.loop(0, keys.shape[0] // TURNS)
    def _(step):
        for turn in range(TURNS):
            keys_across[step * TURNS + turn] = keys[step * TURNS + turn].T

    for copy in copies[11:14]:
        copy.wait()
    for t in range(tiles_ff):
        for part in range(2):
            win_across[t, part] = win[part, pl.ds(t * TILE, LANES), :].T


    def wait_parts(recv_ref, phase, plane):
        arrived = recv_ref.at[plane] if plane != SUMMING else recv_ref.at[plane, pl.ds(0, N - 1)]
        waiter(arrived, 0, sum_sem.at[phase, plane]).wait_recv()

    @pl.when(sums & (me < OWNERS))
    def _():
        qkv_recv[SUMMING, me] = qkv_send[me]
        rest_recv[SUMMING, me] = rest_send[me]
        for plane in (1 - SUMMING, SUMMING):
            wait_parts(rest_recv, 3, plane)
            rest = jnp.sum(rest_recv[plane].astype(F32), axis=0)
            square = rest[SQUARE_ROW - G : SQUARE_ROW - G + 1]
            square = square[:, 0:1] + square[:, LANES // 2 : LANES // 2 + 1]
            scale = lax.rsqrt(square / MODEL_WIDTH + EPSILON)
            wait_parts(qkv_recv, 0, plane)
            total = jnp.sum(qkv_recv[plane].astype(F32), axis=0)
            total = jnp.concatenate([total, rest, jnp.zeros_like(rest)], axis=0) * scale
            rotated = total * cosine + pltpu.roll(total, D // 2, 1) * sine
            tile_out[plane] = jnp.where(iota((2 * G, LANES), 0) <= G, rotated, total).astype(BF16)
            for offset in ALL + [(0, 0)]:
                if offset != (0, 0) or plane != SUMMING:
                    copy_to(
                        tile_out.at[plane, pl.ds(0, G)],
                        q_all.at[me],
                        1 + plane,
                        at(kvp_at(*offset), plane),
                        query_sem.at[my_z],
                    )
            for target in joiners(me):
                copy_to(
                    tile_out.at[plane],
                    tile.at[plane],
                    3 + plane,
                    at(target, SUMMING),
                    tile_sem.at[plane],
                )
        q_all[me] = tile_out[SUMMING, pl.ds(0, G)]

    head_at = iota((G, LANES), 0) * WIDE
    in_block = (lane >= head_at) & (lane < head_at + WIDE)

    def to_column(row):
        return jnp.sum(jnp.where(lane == head_at, row, 0.0), axis=1, keepdims=True)

    factor = D ** (-0.5)
    first = me * (PAGES_HERE * PAGE)

    def attend(requests):
        slots = [[table[p, b] for p in range(PAGES_HERE)] for b in requests]
        queries = [q_all[b] for b in requests]
        scores = [
            [
                jnp.dot(query, keys_across[slot], preferred_element_type=F32)
                for slot in here
            ]
            for query, here in zip(queries, slots)
        ]
        parts = []
        for b, here, products in zip(requests, slots, scores):
            left = lengths[b] - first
            live = [lane + p * PAGE < left for p in range(PAGES_HERE)]
            masked = [jnp.where(ok, s * factor, -1e30) for ok, s in zip(live, products)]
            top = jnp.max(functools.reduce(jnp.maximum, masked), axis=1, keepdims=True)
            weights = [jnp.where(ok, jnp.exp(s - top), 0.0) for ok, s in zip(live, masked)]
            total = jnp.sum(functools.reduce(jnp.add, weights), axis=1, keepdims=True)
            summed = 0.0
            for p in range(PAGES_HERE):
                summed = summed + jnp.dot(
                    weights[p].astype(BF16), values[here[p]], preferred_element_type=F32
                )
            both = jnp.where(lane % WIDE < WIDE // 2, top, total)
            row = jnp.sum(jnp.where(in_block, both, 0.0), axis=0, keepdims=True)
            parts.append((summed.astype(BF16), row))
        for b, (part, row) in zip(requests, parts):
            part_send[b] = part
            stat_send[b] = row

    def send_part(request, target):
        copy_to(
            part_send.at[request],
            part_recv.at[my_c, me],
            5,
            at(target, SUMMING),
            sum_sem.at[1, my_c],
        )
        copy_to(
            stat_send.at[request],
            stat_recv.at[my_c, pl.ds(me, 1)],
            14,
            at(target, SUMMING),
            sum_sem.at[4, my_c],
        )

    for place in range(ROWS):
        row = 0
        for z in range(Z):
            row = jnp.where(my_z == z, NEAREST_ROWS[z][place], row)
        requests = [row * X + x for x in range(X)]
        if place == 0:

            @pl.when(sums & (me < OWNERS))
            def _(row=row):
                waiter(q_all.at[pl.ds(0, X - 1)], 0, query_sem.at[row]).wait_recv()

            @pl.when(jnp.logical_not(sums & (me < OWNERS)))
            def _(row=row):
                waiter(q_all.at[pl.ds(0, X)], 0, query_sem.at[row]).wait_recv()

        else:
            waiter(q_all.at[pl.ds(0, X)], 0, query_sem.at[row]).wait_recv()
        attend(requests)
        for request in requests:
            for target in joiners(request):

                @pl.when((me != target) | (my_c != SUMMING))
                def _(request=request, target=target):
                    send_part(request, target)

    copies[10].wait()

    @pl.when(sums)
    def _():
        part_recv[SUMMING, me] = part_send[my_request]
        stat_recv[SUMMING, pl.ds(me, 1)] = stat_send[my_request]
        for plane in (1 - SUMMING, SUMMING):

            waiter(tile.at[plane], 0, tile_sem.at[plane]).wait_recv()
            known = tile[plane].astype(F32)
            new_key, new_value = known[G : G + 1], known[G + 1 : G + 2]
            own = jnp.sum(known[:G] * new_key, axis=1, keepdims=True) * factor
            own_row = jnp.sum(jnp.where(in_block, own, 0.0), axis=0, keepdims=True)
            wait_parts(stat_recv, 4, plane)
            stats = stat_recv[plane]
            overall = jnp.maximum(jnp.max(stats, axis=0, keepdims=True), own_row)
            carried = jnp.exp(stats - overall)
            totals = pltpu.roll(stats, LANES - WIDE // 2, 1)
            own_row = jnp.exp(own_row - overall)
            total = to_column(jnp.sum(totals * carried, axis=0, keepdims=True) + own_row)
            summed = rounded(to_column(own_row)) * new_value
            carried = [to_column(carried[k : k + 1]) for k in range(N)]
            wait_parts(part_recv, 1, plane)
            for k in range(N):
                summed = summed + part_recv[plane, k].astype(F32) * carried[k]
            joined[plane] = (summed / total).astype(BF16)
            for offset in NEAR + [(0, 0)]:
                if offset != (0, 0) or plane != SUMMING:
                    copy_to(
                        joined.at[plane],
                        attn_all.at[my_request],
                        6 + plane,
                        at(kvp_at(*offset), plane),
                        all_sem.at[0],
                    )
        attn_all[my_request] = joined[SUMMING]
        waiter(attn_all.at[pl.ds(0, len(NEAR))], 0, all_sem.at[0]).wait_recv()

    @pl.when(my_c != SUMMING)
    def _():
        waiter(attn_all, 0, all_sem.at[0]).wait_recv()

    attn_rows[...] = attn_all[...].astype(F32).reshape(B * G, D)
    attn = jnp.concatenate(
        [attn_rows[pl.ds(g, B, stride=G), :].astype(BF16) for g in range(G)], axis=1
    )

    def over_heads(term, send_ref, recv_ref, phase):
        send_ref[...] = term.astype(BF16)
        for offset in HEADS:
            copy_to(send_ref, recv_ref.at[my_head], phase, head_peer(*offset))
        recv_ref[my_head] = term.astype(BF16)
        waiter(recv_ref.at[pl.ds(0, len(HEADS))], phase).wait_recv()
        return jnp.sum(recv_ref[...].astype(F32), axis=0)

    term = jnp.dot(attn, wo[...], preferred_element_type=F32)
    stream = x + over_heads(term, head_send, head_recv, 8)

    square = jnp.sum(stream * stream, axis=1, keepdims=True)
    high = rounded(square)
    column = iota((B, LANES), 1)
    normed = (stream * mlp_gain[...][None, :].astype(F32)).astype(BF16)
    ours = [tiles[step] for step in range(tiles_ff)]

    def make(step):
        for part in range(2):
            product = jnp.dot(normed, win_across[ours[step], part], preferred_element_type=F32)
            rest = jnp.where(column == TILE, high, square - high) if part == 0 else 0.0
            ff_send[ours[step], part] = jnp.where(column < TILE, product, rest).astype(BF16)

    def send(step):
        copy_to(
            ff_send.at[ours[step]],
            ff_recv.at[my_c, me],
            10,
            at(lax.rem(ours[step] * SPREAD, N), SUMMING),
            sum_sem.at[2, my_c],
        )

    start = 0
    for size in GROUPS:
        for step in range(start, start + size):
            make(step)
        for step in range(start, start + size):
            send(step)
        start += size
    make(start)

    @pl.when((my_tile >= tiles_ff) | (my_c != SUMMING))
    def _():
        send(start)

    summing_tile = sums & (my_tile < tiles_ff)

    @pl.when(summing_tile)
    def _():
        ff_recv[SUMMING, me] = ff_send[my_tile]
        for plane in (1 - SUMMING, SUMMING):
            wait_parts(ff_recv, 2, plane)
            both = jnp.sum(ff_recv[plane].astype(F32), axis=0)
            square = both[0][:, TILE : TILE + 1] + both[0][:, TILE + 1 : TILE + 2]
            scale = lax.rsqrt(square / MODEL_WIDTH + EPSILON)
            gate, up = both[0] * scale, both[1] * scale
            active = gate / (1.0 + jnp.exp(-gate)) * up
            units[plane] = jnp.where(column < TILE, active, 0.0).astype(BF16)
            for offset in ALL + [(0, 0)]:
                if offset != (0, 0) or plane != SUMMING:
                    copy_to(
                        units.at[plane],
                        hid_all.at[my_tile],
                        11 + plane,
                        at(kvp_at(*offset), plane),
                        all_sem.at[1],
                    )
        hid_all[my_tile] = units[SUMMING]
        waiter(hid_all.at[pl.ds(0, tiles_ff - 1)], 0, all_sem.at[1]).wait_recv()

    @pl.when(jnp.logical_not(summing_tile))
    def _():
        waiter(hid_all, 0, all_sem.at[1]).wait_recv()

    copies[14].wait()
    term = 0.0
    for t in range(tiles_ff):
        term = term + jnp.dot(
            hid_all[t], wdown[pl.ds(t * TILE, LANES), :], preferred_element_type=F32
        )
    out_ref[...] = (stream + over_heads(term, last_send, last_recv, 9)).astype(BF16)

    @pl.when(sums & (me < OWNERS))
    def _():
        waiter(qkv_recv.at[0, pl.ds(0, OWNERS - 1)], 0).wait_send()
        waiter(rest_recv.at[0, pl.ds(0, OWNERS - 1)], 13).wait_send()
        for plane in range(C):
            count = N if plane != SUMMING else N - 1
            waiter(qkv_recv.at[0, pl.ds(0, count)], 1 + plane).wait_send()
            waiter(tile_out, 3 + plane).wait_send()

    @pl.when(jnp.logical_not(sums & (me < OWNERS)))
    def _():
        waiter(qkv_recv.at[0, pl.ds(0, OWNERS)], 0).wait_send()
        waiter(rest_recv.at[0, pl.ds(0, OWNERS)], 13).wait_send()

    @pl.when(sums)
    def _():
        waiter(part_recv.at[0, pl.ds(0, N - 1)], 5).wait_send()
        waiter(stat_recv.at[0, pl.ds(0, N - 1)], 14).wait_send()
        for plane in range(C):
            count = len(NEAR) + (plane != SUMMING)
            waiter(attn_all.at[pl.ds(0, count)], 6 + plane).wait_send()

    @pl.when(my_c != SUMMING)
    def _():
        waiter(part_recv.at[0], 5).wait_send()
        waiter(stat_recv.at[0], 14).wait_send()

    waiter(head_recv.at[pl.ds(0, len(HEADS))], 8).wait_send()
    waiter(last_recv.at[pl.ds(0, len(HEADS))], 9).wait_send()

    @pl.when(summing_tile)
    def _():
        waiter(ff_recv.at[0, pl.ds(0, tiles_ff - 1)], 10).wait_send()
        for plane in range(C):
            count = N if plane != SUMMING else N - 1
            waiter(ff_recv.at[0, pl.ds(0, count), 0], 11 + plane).wait_send()

    @pl.when(jnp.logical_not(summing_tile))
    def _():
        waiter(ff_recv.at[0, pl.ds(0, tiles_ff)], 10).wait_send()


def on_device(
    hidden_in,
    attn_gain,
    query_key_value_weight,
    k_cache,
    value_cache,
    page_table,
    lengths,
    output_weight,
    mlp_gain,
    w_in,
    w_down,
):
    width = hidden_in.shape[1]
    ff = w_down.shape[0]
    tiles_ff = -(-ff // TILE)
    half = D // 2
    inverse = ROPE_BASE ** (-np.arange(half, dtype=np.float64) * (2.0 / D))
    inverse = np.broadcast_to(np.concatenate([inverse, inverse]), (8, D)).astype(np.float32)
    slots = k_cache.shape[1]
    return pl.pallas_call(
        functools.partial(kernel, tiles_ff, ff),
        out_shape=pltpu.VMEM((B, width), BF16),
        in_specs=[pl.BlockSpec(memory_space=pl.ANY)] * 12,
        out_specs=pl.BlockSpec(memory_space=pltpu.VMEM),
        scratch_shapes=[
            pltpu.VMEM((B, width), BF16),
            pltpu.VMEM((width,), BF16),
            pltpu.VMEM((width,), BF16),
            pltpu.VMEM((8, D), F32),
            pltpu.SMEM((PAGES_HERE, B), jnp.int32),
            pltpu.SMEM((B,), jnp.int32),
            pltpu.VMEM((width, VECTORS * D), BF16),
            pltpu.VMEM((slots, PAGE, D), BF16),
            pltpu.VMEM((slots, PAGE, D), BF16),
            pltpu.VMEM((slots, D, PAGE), BF16),
            pltpu.VMEM((G * D, width), BF16),
            pltpu.VMEM((2, (tiles_ff - 1) * TILE + LANES, width), BF16),
            pltpu.VMEM((tiles_ff, 2, width, LANES), BF16),
            pltpu.VMEM(((tiles_ff - 1) * TILE + LANES, width), BF16),
            pltpu.VMEM((B * 2 * G, D), F32),
            pltpu.VMEM((B, G, D), BF16),
            pltpu.VMEM((C, N, G, D), BF16),
            pltpu.VMEM((B, REST, D), BF16),
            pltpu.VMEM((C, N, REST, D), BF16),
            pltpu.VMEM((B, G, D), BF16),
            pltpu.VMEM((C, 2 * G, D), BF16),
            pltpu.VMEM((C, 2 * G, D), BF16),
            pltpu.VMEM((B, G, D), BF16),
            pltpu.VMEM((C, N, G, D), BF16),
            pltpu.VMEM((B, 1, LANES), F32),
            pltpu.VMEM((C, N, LANES), F32),
            pltpu.VMEM((C, G, D), BF16),
            pltpu.VMEM((B, G, D), BF16),
            pltpu.VMEM((B * G, D), F32),
            pltpu.VMEM((B, width), BF16),
            pltpu.VMEM((H, B, width), BF16),
            pltpu.VMEM((tiles_ff, 2, B, LANES), BF16),
            pltpu.VMEM((C, N, 2, B, LANES), BF16),
            pltpu.VMEM((C, B, LANES), BF16),
            pltpu.VMEM((tiles_ff, B, LANES), BF16),
            pltpu.VMEM((B, width), BF16),
            pltpu.VMEM((H, B, width), BF16),
            pltpu.SMEM((N,), jnp.int32),
            pltpu.SMEM((N,), jnp.int32),
            pltpu.SemaphoreType.DMA((15,)),
            pltpu.SemaphoreType.DMA((ROWS,)),
            pltpu.SemaphoreType.DMA((5, C)),
            pltpu.SemaphoreType.DMA((C,)),
            pltpu.SemaphoreType.DMA((2,)),
            pltpu.SemaphoreType.DMA((15,)),
            pltpu.SemaphoreType.DMA((15,)),
        ],
        compiler_params=pltpu.CompilerParams(collective_id=0, has_side_effects=True),
    )(
        hidden_in,
        attn_gain,
        query_key_value_weight.transpose(1, 0, 2)[0],
        k_cache[0],
        value_cache[0],
        page_table.T,
        lengths,
        output_weight[0],
        mlp_gain,
        w_in.transpose(1, 2, 0),
        w_down,
        jnp.asarray(inverse),
    )


def solution(mesh):
    return jax.shard_map(
        on_device,
        mesh=mesh,
        in_specs=(
            P(None, "kvp"),
            P("kvp"),
            P("kvp", "head", None),
            P("head", "kvp", None, None),
            P("head", "kvp", None, None),
            P(None, "kvp"),
            P(),
            P("head", None, "kvp"),
            P("kvp"),
            P("kvp", None, "head"),
            P("head", "kvp"),
        ),
        out_specs=P(None, "kvp"),
        check_vma=False,
    )
```
